256 devices in a mesh: grp: 8 (over x_lo, y), tp: 32 (over x_hi, z, core).
Axes of the slice: x: 4 (x_hi: 2, x_lo: 2; x = x_hi * 2 + x_lo), y: 4, z: 8, core: 2. Of those that a mesh axis runs over, the one named last changes fastest.
Arguments:
- batch_sizes: int32 [8], P('grp'), may hold values from 1 to 16
- seq_lens: int32 [8, 16], P('grp'), may hold values from 1 to 8192
- page_table: int32 [8, 16, 512], P('grp', None, 'tp'), may hold values from 0 to 255, as said below
- queries: bfloat16 [8, 16, 4096], P('grp', None, 'tp'), may hold values from -4 to 14
- kv_pool: bfloat16 [8, 8192, 16, 1024], P('grp', 'tp'), may hold values from -7 to 7
- new_kv: bfloat16 [8, 16, 1024], P('grp'), may hold values from -6 to 6
- out_weight: bfloat16 [4096, 2880], P('tp', 'grp'), may hold values from -0.375 to 0.375
Outputs:
- mixed: float32 [8, 16, 2880], P('grp')
The draws below stay inside these ranges and needn't reach their ends.
Inputs may be any that keep to these rules, and one draw needn't show every extreme that they name: `batch_sizes`: slots below a group's batch size are live; the others are empty and their outputs are zero. `seq_lens`: entries of empty slots are drawn but unused. `page_table`: for every group g and every t, the entries [g, :, t * 16 to (t + 1) * 16 - 1] are a permutation of 0 to 255.
All inputs are finite; a program needn't handle non-finite values.
Results may differ from the reference program's by a relative error of at most 0.007.
Values may be sent and summed in bfloat16 or wider, within the bound.
No kernel may reach another device: no remote copies, remote signals or barrier semaphores. Data moves between devices by JAX's collectives and lax.ppermute only.
A program may use at most 64 MiB of HBM per device.

```python
import jax
import jax.numpy as jnp
from jax import lax

D = 2880
HEADS = 64
KV_HEADS = 8
HD = 64
PAGE = 16
PAGES_DEV = 16
SLOTS = 16
GROUPS = 8
POOL_DEV = 256
MAX_LEN = 8192
N_TP = 32


def draw_page_table(key, part):
    subkeys = jax.random.split(jax.random.fold_in(key, 101), GROUPS * N_TP)
    orders = jax.vmap(lambda single: jax.random.permutation(single, POOL_DEV))(subkeys)
    orders = orders.reshape(GROUPS, N_TP, SLOTS, PAGES_DEV).transpose(0, 2, 1, 3)
    return orders.reshape(GROUPS, SLOTS, N_TP * PAGES_DEV).astype(jnp.int32)


def draw_queries(key, part):
    noise = jax.random.normal(jax.random.fold_in(key, 11), (GROUPS, SLOTS, HEADS * HD), jnp.float32)
    noise = jnp.clip(noise, -4.0, 4.0)
    return noise.astype(jnp.bfloat16)


def draw_kv_pool(key, part):
    extent = (GROUPS, N_TP * POOL_DEV, PAGE, 2 * KV_HEADS * HD)
    column = jnp.arange(2 * KV_HEADS * HD)
    key_column = column < KV_HEADS * HD
    noise = jnp.clip(jax.random.normal(jax.random.fold_in(key, 22), extent, jnp.float32), -4.0, 4.0)
    noise = noise * jnp.where(key_column, 1.5, 1.0)
    return noise.astype(jnp.bfloat16)


def set_ends(values, rng, smallest, top_value):
    spot = [jax.random.randint(jax.random.fold_in(rng, axis), (), 0, length) for axis, length in enumerate(values.shape)]
    main_axis = values.shape.index(max(values.shape))
    beside = spot[:main_axis] + [(spot[main_axis] + 1) % values.shape[main_axis]] + spot[main_axis + 1:]
    return values.at[tuple(spot)].set(smallest).at[tuple(beside)].set(top_value)


def block_levels(key, shape, cuts, low, top_value):
    def one(dim, shards_of):
        draws = jax.random.uniform(jax.random.fold_in(jax.random.fold_in(key, 6), dim), (shards_of,), jnp.float32, low / len(cuts), top_value / len(cuts))
        return jnp.repeat(jnp.exp(draws), shape[dim] // shards_of).reshape((-1,) + (1,) * (len(shape) - dim - 1))

    factor_of = one(*cuts[0])
    for cut in cuts[1:]:
        factor_of = factor_of * one(*cut)
    return factor_of


def scatter_about(rng, dims, spread, bound, pieces=(), kind=jnp.bfloat16):
    values = jax.random.normal(rng, dims, jnp.float32) * spread
    if len(pieces) > 0:
        values = block_levels(rng, dims, pieces, -0.22, 0.18) * values
    return jnp.clip(values, min=-bound, max=bound).astype(kind)


def setup_inputs(seed: int = 0) -> dict:
    streams_of = jax.random.split(jax.random.key(seed), 8)
    batch_sizes = set_ends(jax.random.randint(streams_of[0], (GROUPS,), 1, SLOTS + 1), jax.random.fold_in(streams_of[0], 1), 1, SLOTS).astype(jnp.int32)
    seq_lens = set_ends(jax.random.randint(streams_of[1], (GROUPS, SLOTS), 1, MAX_LEN + 1), jax.random.fold_in(streams_of[1], 1), 1, MAX_LEN).astype(jnp.int32)
    page_table = draw_page_table(jax.random.fold_in(streams_of[7], 71), 0)
    queries = draw_queries(jax.random.fold_in(streams_of[7], 71), 0)
    kv_pool = draw_kv_pool(jax.random.fold_in(streams_of[7], 71), 0)
    new_kv = scatter_about(streams_of[5], (GROUPS, SLOTS, 2 * KV_HEADS * HD), 1.0, 6.0, ((0, 8),))
    out_weight = scatter_about(streams_of[6], (HEADS * HD, D), (HEADS * HD // 16) ** -0.5, 0.375, ((0, 32), (1, 8)))
    return dict(batch_sizes=batch_sizes, seq_lens=seq_lens, page_table=page_table, queries=queries, kv_pool=kv_pool, new_kv=new_kv, out_weight=out_weight)


PRECISE = lax.Precision.HIGHEST
NEG_BIG = -1.0e30


def slot_output(query_row, length, entries, group_pool, fresh_row):
    entry_ids = jnp.arange(N_TP * PAGES_DEV, dtype=jnp.int32)
    owner_dev = entry_ids // PAGES_DEV
    within = entry_ids % PAGES_DEV
    pool_rows = owner_dev * POOL_DEV + entries.astype(jnp.int32)
    page_number = within * N_TP + owner_dev
    position = (page_number[:, None] * PAGE + jnp.arange(PAGE, dtype=jnp.int32)[None, :]).reshape(-1)
    tokens = group_pool[pool_rows].reshape(N_TP * PAGES_DEV * PAGE, 2 * KV_HEADS * HD).astype(jnp.float32)
    keys_all = tokens[:, : KV_HEADS * HD].reshape(-1, KV_HEADS, HD)
    values_all = tokens[:, KV_HEADS * HD:].reshape(-1, KV_HEADS, HD)
    grouped = query_row.astype(jnp.float32).reshape(KV_HEADS, HEADS // KV_HEADS, HD)
    score_scale = HD ** -0.5
    scores = jnp.einsum("kgd,tkd->kgt", grouped, keys_all, precision=PRECISE) * score_scale
    valid_mask = (position < length)[None, None, :]
    scores = jnp.where(valid_mask, scores, NEG_BIG)
    fresh = fresh_row.astype(jnp.float32)
    new_key = fresh[: KV_HEADS * HD].reshape(KV_HEADS, HD)
    new_value = fresh[KV_HEADS * HD:].reshape(KV_HEADS, HD)
    own_score = jnp.einsum("kgd,kd->kg", grouped, new_key, precision=PRECISE) * score_scale
    top_score = jnp.maximum(jnp.max(scores, axis=2), own_score)
    weights = jnp.where(valid_mask, jnp.exp(scores - top_score[:, :, None]), 0.0)
    rounded = lax.optimization_barrier(weights.astype(jnp.bfloat16)).astype(jnp.float32)
    own_weight = jnp.exp(own_score - top_score)
    numerator = jnp.einsum("kgt,tkd->kgd", rounded, values_all, precision=PRECISE)
    numerator = numerator + own_weight[:, :, None] * new_value[:, None, :]
    denominator = jnp.sum(weights, axis=2) + own_weight
    return (numerator / denominator[:, :, None]).reshape(HEADS * HD)


def group_output(inputs):
    live_count, lengths, page_ids, group_queries, group_pool, group_new = inputs

    def one_slot(slot_item):
        query_row, length, entries, fresh_row = slot_item
        return slot_output(query_row, length, entries, group_pool, fresh_row)

    slot_rows = lax.map(one_slot, (group_queries, lengths, page_ids, group_new))
    live_mask = jnp.arange(SLOTS, dtype=jnp.int32) < live_count
    return jnp.where(live_mask[:, None], slot_rows, 0.0).astype(jnp.bfloat16)


def reference(batch_sizes, seq_lens, page_table, queries, kv_pool, new_kv, out_weight):
    attended = lax.map(group_output, (batch_sizes, seq_lens, page_table, queries, kv_pool, new_kv))
    flat_rows = attended.reshape(GROUPS * SLOTS, HEADS * HD)
    mixed = jnp.dot(flat_rows, out_weight, preferred_element_type=jnp.float32)
    return mixed.reshape(GROUPS, SLOTS, D).astype(jnp.float32)
```

```python
import functools

import jax
import jax.numpy as jnp
from jax import lax
from jax.experimental import pallas as pl
from jax.experimental.pallas import tpu as pltpu
from jax.sharding import PartitionSpec as P

HEADS = 64
KV_HEADS = 8
HD = 64
LANES = 128
NEG_BIG = -1e30
BF = jnp.bfloat16
F32 = jnp.float32
STAT_ROW = 16
MSG_ROWS = 24
INTERPRET = False


def lane_iota(rows):
    return lax.broadcasted_iota(jnp.int32, (rows, LANES), 1)


def roll_lanes(x, shift):
    return pltpu.roll(x, shift, 1)


def split_bf(x):
    hi = x.astype(BF)
    lo = (x - hi.astype(F32)).astype(BF)
    return hi, lo


def attend_kernel(info_ref, lens_ref, table_ref, q_ref, kv_ref, out_ref, q_scr, num_scr, stat_scr):
    n_tp, slots, _ = q_ref.shape
    pages = table_ref.shape[1]
    page_len = kv_ref.shape[1]
    kv_cols = KV_HEADS * HD
    tokens = pages * page_len
    live_count = info_ref[0]
    tp_index = info_ref[1]
    q_scr[...] = (q_ref[...].astype(F32) * HD**-0.5).reshape(n_tp * slots, LANES)
    num_scr[...] = jnp.zeros_like(num_scr)
    low_half = lane_iota(n_tp) < HD
    own_block = (
        lax.broadcasted_iota(jnp.int32, (n_tp, kv_cols), 1) // HD
        == lax.broadcasted_iota(jnp.int32, (n_tp, kv_cols), 0) // (n_tp // KV_HEADS)
    )
    column = lax.broadcasted_iota(jnp.int32, (HEADS, tokens), 1)
    position = (column // page_len) * (page_len * n_tp) + tp_index * page_len + column % page_len
    lane = lane_iota(HEADS)

    def one_slot(slot, state):
        tops, sums = state
        x = q_scr[pl.ds(slot, n_tp, stride=slots), :]
        turned = roll_lanes(x, HD)
        even = jnp.where(low_half, x, turned)
        odd = jnp.where(low_half, turned, x)
        wide = [jnp.where(own_block, jnp.concatenate([h] * 4, axis=1), 0.0) for h in (even, odd)]
        spread = jnp.concatenate(wide, axis=0).astype(BF)
        ids = [table_ref[slot, i] for i in range(pages)]
        keys = jnp.concatenate([kv_ref[i, :, 0:kv_cols] for i in ids], axis=0)
        values = jnp.concatenate([kv_ref[i, :, kv_cols : 2 * kv_cols] for i in ids], axis=0)
        scores = lax.dot_general(
            spread, keys, (((1,), (1,)), ((), ())), preferred_element_type=F32
        )
        live = position < lens_ref[slot]
        scores = jnp.where(live, scores, NEG_BIG)
        top = jnp.max(scores, axis=1, keepdims=True)
        top = (top + jnp.abs(top) * 2.0**-7).astype(BF).astype(F32)
        weights = jnp.where(live, jnp.exp(scores - top), 0.0)
        total = jnp.sum(weights, axis=1, keepdims=True)
        mixed = jnp.dot(weights.astype(BF), values, preferred_element_type=F32)
        folded = []
        for part in (mixed[:n_tp], mixed[n_tp:]):
            part = jnp.where(own_block, part, 0.0)
            part = sum(part[:, i * LANES : (i + 1) * LANES] for i in range(4))
            folded.append(part + roll_lanes(part, HD))
        num_scr[pl.ds(pl.multiple_of(slot * n_tp, n_tp), n_tp), :] = jnp.where(
            low_half, folded[0], folded[1]
        )
        here = lane == slot
        return jnp.where(here, top, tops), jnp.where(here, total, sums)

    start = (
        jnp.where(lane < slots, NEG_BIG, 0.0).astype(F32),
        jnp.zeros((HEADS, LANES), F32),
    )
    tops, sums = lax.fori_loop(0, live_count, one_slot, start)
    hi, lo = split_bf(sums)
    packed = tops + roll_lanes(hi.astype(F32), slots) + roll_lanes(lo.astype(F32), 2 * slots)
    stat_scr[...] = packed[:n_tp] + roll_lanes(packed[n_tp:], HD)
    for t in range(n_tp):
        out_ref[t, 0:slots, :] = num_scr[pl.ds(t, slots, stride=n_tp), :].astype(BF)
        out_ref[t, STAT_ROW:MSG_ROWS, :] = jnp.broadcast_to(
            stat_scr[t : t + 1, :], (MSG_ROWS - STAT_ROW, LANES)
        ).astype(BF)


def combine_kernel(info_ref, msg_ref, q_ref, new_ref, *rest):
    weight_refs, out_ref = rest[:-1], rest[-1]
    n_tp = msg_ref.shape[0]
    slots = q_ref.shape[0]
    live_count = info_ref[0]
    tp_index = info_ref[1]
    grp_index = info_ref[2]
    blocks = len(weight_refs)
    width = weight_refs[0].shape[1]
    ones_block = (
        lax.broadcasted_iota(jnp.int32, (LANES, LANES), 0) // HD
        == lax.broadcasted_iota(jnp.int32, (LANES, LANES), 1) // HD
    ).astype(F32).astype(BF)
    rows8 = MSG_ROWS - STAT_ROW
    stats = [msg_ref[t, STAT_ROW:MSG_ROWS, :].astype(F32) for t in range(n_tp)]
    top = functools.reduce(jnp.maximum, stats)
    scale = [jnp.exp(s - top) for s in stats]
    sums = sum(
        w * (roll_lanes(s, LANES - slots) + roll_lanes(s, LANES - 2 * slots))
        for w, s in zip(scale, stats)
    )
    sub = lax.broadcasted_iota(jnp.int32, (rows8, LANES), 0)
    within = lane_iota(rows8) % HD
    picks = [within == sub + rows8 * i for i in range(slots // rows8)]
    picked = jnp.concatenate(
        [jnp.where(p, v, 0.0) for v in (*scale, top, sums) for p in picks], axis=0
    )
    hi, lo = split_bf(picked)
    spread = jnp.dot(hi, ones_block, preferred_element_type=F32) + jnp.dot(
        lo, ones_block, preferred_element_type=F32
    )
    top_all = spread[n_tp * slots : (n_tp + 1) * slots]
    sum_all = spread[(n_tp + 1) * slots :]
    numerator = sum(
        msg_ref[t, 0:slots, :].astype(F32) * spread[t * slots : (t + 1) * slots]
        for t in range(n_tp)
    )

    kv_head = tp_index // (n_tp // KV_HEADS)
    low_half = lane_iota(slots) < HD

    def own_columns(first):
        at = pl.multiple_of(first + (kv_head // 2) * LANES, LANES)
        block = new_ref[:, pl.ds(at, LANES)].astype(F32)
        turned = roll_lanes(block, HD)
        low = jnp.where(low_half, block, turned)
        high = jnp.where(low_half, turned, block)
        return jnp.where(kv_head % 2 == 0, low, high)

    new_key = own_columns(0)
    new_value = own_columns(KV_HEADS * HD)
    products = q_ref[...].astype(F32) * HD**-0.5 * new_key
    hi, lo = split_bf(products)
    self_score = jnp.dot(hi, ones_block, preferred_element_type=F32) + jnp.dot(
        lo, ones_block, preferred_element_type=F32
    )
    final_top = jnp.maximum(top_all, self_score)
    cached = jnp.exp(top_all - final_top)
    fresh = jnp.exp(self_score - final_top)
    attended = (numerator * cached + new_value * fresh) / (sum_all * cached + fresh)
    slot = lax.broadcasted_iota(jnp.int32, (slots, LANES), 0)
    attended = jnp.where(slot < live_count, attended, 0.0).astype(BF)
    parts = n_tp // blocks
    rows = slots // parts
    for k in range(blocks):
        share = jnp.dot(attended, weight_refs[k][...], preferred_element_type=F32).astype(BF)
        block = lax.rem(grp_index + blocks - k, blocks)
        for i in range(parts):
            out_ref[block * parts + i, :, 0:width] = share[i * rows : (i + 1) * rows]


def total_kernel(in_ref, out_ref):
    n_tp = in_ref.shape[0]
    total = sum(in_ref[t].astype(F32) for t in range(n_tp)).astype(BF)
    for t in range(n_tp):
        out_ref[t] = total


def finish_kernel(in_ref, out_ref):
    n_tp, rows, _ = in_ref.shape
    parts = out_ref.shape[1] // rows
    blocks = n_tp // parts
    width = out_ref.shape[2] // blocks
    for b in range(blocks):
        for i in range(parts):
            out_ref[0, i * rows : (i + 1) * rows, b * width : (b + 1) * width] = in_ref[
                b * parts + i, :, 0:width
            ].astype(F32)


SMEM = functools.partial(pl.BlockSpec, memory_space=pltpu.SMEM)
VMEM = functools.partial(pl.BlockSpec, memory_space=pltpu.VMEM)


def attend(info, lens, table, gathered, pool):
    n_tp, slots, _ = gathered.shape
    return pl.pallas_call(
        attend_kernel,
        out_shape=jax.ShapeDtypeStruct((n_tp, MSG_ROWS, LANES), BF),
        in_specs=[SMEM(), SMEM(), SMEM(), VMEM(), VMEM()],
        out_specs=VMEM(),
        scratch_shapes=[
            pltpu.VMEM((n_tp * slots, LANES), F32),
            pltpu.VMEM((slots * n_tp, LANES), F32),
            pltpu.VMEM((n_tp, LANES), F32),
        ],
        interpret=INTERPRET,
        name="attend",
    )(info, lens, table, gathered, pool)


def combine(info, message, own, fresh, weights):
    n_tp = message.shape[0]
    slots = own.shape[0]
    rows = slots * len(weights) // n_tp
    width = -(-weights[0].shape[1] // LANES) * LANES
    return pl.pallas_call(
        combine_kernel,
        out_shape=jax.ShapeDtypeStruct((n_tp, rows, width), BF),
        in_specs=[SMEM()] + [VMEM()] * (3 + len(weights)),
        out_specs=VMEM(),
        interpret=INTERPRET,
        name="combine",
    )(info, message, own, fresh, *weights)


def total_copies(pieces):
    return pl.pallas_call(
        total_kernel,
        out_shape=jax.ShapeDtypeStruct(pieces.shape, BF),
        in_specs=[VMEM()],
        out_specs=VMEM(),
        interpret=INTERPRET,
        name="total",
    )(pieces)


def finish(pieces, slots, width):
    return pl.pallas_call(
        finish_kernel,
        out_shape=jax.ShapeDtypeStruct((1, slots, width), F32),
        in_specs=[VMEM()],
        out_specs=VMEM(),
        interpret=INTERPRET,
        name="finish",
    )(pieces)


def exchange(pieces, axis):
    return lax.all_to_all(pieces, axis, split_axis=0, concat_axis=0, tiled=True)


def local(batch_sizes, seq_lens, page_table, queries, kv_pool, new_kv, out_weight):
    n_tp = lax.axis_size("tp")
    n_grp = lax.axis_size("grp")
    tp_index = lax.axis_index("tp")
    grp_index = lax.axis_index("grp")
    own = queries[0]
    slots = own.shape[0]
    info = jnp.stack([batch_sizes[0], tp_index.astype(jnp.int32), grp_index.astype(jnp.int32)])
    weights = [out_weight]
    for k in range(1, n_grp):
        ring = [(i, (i + k) % n_grp) for i in range(n_grp)]
        weights.append(lax.ppermute(out_weight, "grp", ring))
    gathered = exchange(jnp.broadcast_to(own, (n_tp, *own.shape)), "tp")
    message = attend(info, seq_lens[0], page_table[0], gathered, kv_pool[0])
    received = exchange(message, "tp")
    shares = combine(info, received, own, new_kv[0], weights)
    totals = total_copies(exchange(shares, "tp"))
    return finish(exchange(totals, "tp"), slots, n_grp * out_weight.shape[1])


def solution(mesh):
    return jax.shard_map(
        local,
        mesh=mesh,
        in_specs=(
            P("grp"),
            P("grp", None),
            P("grp", None, "tp"),
            P("grp", None, "tp"),
            P("grp", "tp", None, None),
            P("grp", None, None),
            P("tp", "grp"),
        ),
        out_specs=P("grp", None, None),
        check_vma=False,
    )
```

```python
import functools

import jax
import jax.numpy as jnp
from jax import lax
from jax.experimental import pallas as pl
from jax.experimental.pallas import tpu as pltpu
from jax.sharding import PartitionSpec as P

HEADS = 64
KV_HEADS = 8
HD = 64
LANES = 128
NEG_BIG = -1e30
BF = jnp.bfloat16
F32 = jnp.float32
STAT_ROW = 16
MSG_ROWS = 24
INTERPRET = False
STEPS = (4, 1, 2)
UNROLL = 2
AHEAD = 2


def lane_iota(rows):
    return lax.broadcasted_iota(jnp.int32, (rows, LANES), 1)


def roll_lanes(x, shift):
    return pltpu.roll(x, shift, 1)


def split_bf(x):
    hi = x.astype(BF)
    lo = (x - hi.astype(F32)).astype(BF)
    return hi, lo


def attend_kernel(
    info_ref, lens_ref, table_ref, q_ref, pool_ref, out_ref, kv_scr, q_scr, num_scr, stat_scr, sems
):
    n_tp, slots, _ = q_ref.shape
    pages = table_ref.shape[1]
    page_len = pool_ref.shape[1]
    kv_cols = KV_HEADS * HD
    tokens = pages * page_len
    live_count = info_ref[0]
    tp_index = info_ref[1]
    steps = (live_count + UNROLL - 1) // UNROLL

    def load_pages(slot):
        for i in range(pages):
            pltpu.make_async_copy(
                pool_ref.at[table_ref[slot, i]], kv_scr.at[slot, i], sems.at[slot]
            ).start()

    def wait_pages(slot):
        pltpu.make_async_copy(
            pool_ref.at[pl.ds(0, pages)], kv_scr.at[slot], sems.at[slot]
        ).wait()

    for step in range(AHEAD):

        @pl.when(step < steps)
        def _():
            for i in range(UNROLL):
                load_pages(step * UNROLL + i)

    q_scr[...] = (q_ref[...].astype(F32) * HD**-0.5).reshape(n_tp * slots, LANES)
    num_scr[...] = jnp.zeros_like(num_scr)
    low_half = lane_iota(n_tp) < HD
    own_block = (
        lax.broadcasted_iota(jnp.int32, (n_tp, kv_cols), 1) // HD
        == lax.broadcasted_iota(jnp.int32, (n_tp, kv_cols), 0) // (n_tp // KV_HEADS)
    )
    column = lax.broadcasted_iota(jnp.int32, (HEADS, tokens), 1)
    position = (column // page_len) * (page_len * n_tp) + tp_index * page_len + column % page_len
    lane = lane_iota(HEADS)

    def slot_queries(slot):
        x = q_scr[pl.ds(slot, n_tp, stride=slots), :]
        turned = roll_lanes(x, HD)
        even = jnp.where(low_half, x, turned)
        odd = jnp.where(low_half, turned, x)
        wide = [jnp.where(own_block, jnp.concatenate([h] * 4, axis=1), 0.0) for h in (even, odd)]
        return jnp.concatenate(wide, axis=0).astype(BF)

    def slot_scores(slot):
        keys = kv_scr[slot, :, :, 0:kv_cols].reshape(tokens, kv_cols)
        return lax.dot_general(
            slot_queries(slot), keys, (((1,), (1,)), ((), ())), preferred_element_type=F32
        )

    def slot_weights(slot, scores):
        live = position < jnp.where(slot < live_count, lens_ref[slot], 0)
        scores = jnp.where(live, scores, NEG_BIG)
        top = jnp.max(scores, axis=1, keepdims=True)
        top = (top + jnp.abs(top) * 2.0**-7).astype(BF).astype(F32)
        weights = jnp.where(live, jnp.exp(scores - top), 0.0)
        return top, jnp.sum(weights, axis=1, keepdims=True), weights.astype(BF)

    def slot_values(slot, weights):
        values = kv_scr[slot, :, :, kv_cols : 2 * kv_cols].reshape(tokens, kv_cols)
        mixed = jnp.dot(weights, values, preferred_element_type=F32)
        folded = []
        for part in (mixed[:n_tp], mixed[n_tp:]):
            part = jnp.where(own_block, part, 0.0)
            part = sum(part[:, i * LANES : (i + 1) * LANES] for i in range(4))
            folded.append(part + roll_lanes(part, HD))
        num_scr[pl.ds(pl.multiple_of(slot * n_tp, n_tp), n_tp), :] = jnp.where(
            low_half, folded[0], folded[1]
        )

    def some_slots(step, state):
        tops, sums = state
        group = [step * UNROLL + i for i in range(UNROLL)]

        @pl.when(step + AHEAD < steps)
        def _():
            for slot in group:
                load_pages(slot + AHEAD * UNROLL)

        for slot in group:
            wait_pages(slot)
        scores = [slot_scores(slot) for slot in group]
        parts = [slot_weights(slot, s) for slot, s in zip(group, scores)]
        for slot, (top, total, weights) in zip(group, parts):
            slot_values(slot, weights)
            here = lane == slot
            tops = jnp.where(here, top, tops)
            sums = jnp.where(here, total, sums)
        return tops, sums

    start = (
        jnp.where(lane < slots, NEG_BIG, 0.0).astype(F32),
        jnp.zeros((HEADS, LANES), F32),
    )
    tops, sums = lax.fori_loop(0, steps, some_slots, start)
    hi, lo = split_bf(sums)
    packed = tops + roll_lanes(hi.astype(F32), slots) + roll_lanes(lo.astype(F32), 2 * slots)
    stat_scr[...] = packed[:n_tp] + roll_lanes(packed[n_tp:], HD)
    for t in range(n_tp):
        out_ref[t, 0:slots, :] = num_scr[pl.ds(t, slots, stride=n_tp), :].astype(BF)
        out_ref[t, STAT_ROW:MSG_ROWS, :] = jnp.broadcast_to(
            stat_scr[t : t + 1, :], (MSG_ROWS - STAT_ROW, LANES)
        ).astype(BF)


def combine_kernel(info_ref, msg_ref, q_ref, new_ref, half_ref, rest_ref, out_ref):
    n_tp = msg_ref.shape[0]
    slots = q_ref.shape[0]
    live_count = info_ref[0]
    tp_index = info_ref[1]
    grp_index = info_ref[2]
    blocks = 2 ** len(STEPS)
    width = half_ref.shape[0] * 2 // blocks
    ones_block = (
        lax.broadcasted_iota(jnp.int32, (LANES, LANES), 0) // HD
        == lax.broadcasted_iota(jnp.int32, (LANES, LANES), 1) // HD
    ).astype(F32).astype(BF)
    rows8 = MSG_ROWS - STAT_ROW
    stats = [msg_ref[t, STAT_ROW:MSG_ROWS, :].astype(F32) for t in range(n_tp)]
    top = functools.reduce(jnp.maximum, stats)
    scale = [jnp.exp(s - top) for s in stats]
    sums = sum(
        w * (roll_lanes(s, LANES - slots) + roll_lanes(s, LANES - 2 * slots))
        for w, s in zip(scale, stats)
    )
    sub = lax.broadcasted_iota(jnp.int32, (rows8, LANES), 0)
    within = lane_iota(rows8) % HD
    picks = [within == sub + rows8 * i for i in range(slots // rows8)]
    picked = jnp.concatenate(
        [jnp.where(p, v, 0.0) for v in (*scale, top, sums) for p in picks], axis=0
    )
    hi, lo = split_bf(picked)
    spread = jnp.dot(hi, ones_block, preferred_element_type=F32) + jnp.dot(
        lo, ones_block, preferred_element_type=F32
    )
    top_all = spread[n_tp * slots : (n_tp + 1) * slots]
    sum_all = spread[(n_tp + 1) * slots :]
    numerator = sum(
        msg_ref[t, 0:slots, :].astype(F32) * spread[t * slots : (t + 1) * slots]
        for t in range(n_tp)
    )

    kv_head = tp_index // (n_tp // KV_HEADS)
    low_half = lane_iota(slots) < HD

    def own_columns(first):
        at = pl.multiple_of(first + (kv_head // 2) * LANES, LANES)
        block = new_ref[:, pl.ds(at, LANES)].astype(F32)
        turned = roll_lanes(block, HD)
        low = jnp.where(low_half, block, turned)
        high = jnp.where(low_half, turned, block)
        return jnp.where(kv_head % 2 == 0, low, high)

    new_key = own_columns(0)
    new_value = own_columns(KV_HEADS * HD)
    products = q_ref[...].astype(F32) * HD**-0.5 * new_key
    hi, lo = split_bf(products)
    self_score = jnp.dot(hi, ones_block, preferred_element_type=F32) + jnp.dot(
        lo, ones_block, preferred_element_type=F32
    )
    final_top = jnp.maximum(top_all, self_score)
    cached = jnp.exp(top_all - final_top)
    fresh = jnp.exp(self_score - final_top)
    attended = (numerator * cached + new_value * fresh) / (sum_all * cached + fresh)
    slot = lax.broadcasted_iota(jnp.int32, (slots, LANES), 0)
    attended = jnp.where(slot < live_count, attended, 0.0).astype(BF)
    parts = n_tp // blocks
    rows = slots // parts
    for k in range(blocks):
        source = half_ref if k < blocks // 2 else rest_ref
        first = k % (blocks // 2) * width
        share = lax.dot_general(
            attended,
            source[first : first + width, :],
            (((1,), (1,)), ((), ())),
            preferred_element_type=F32,
        ).astype(BF)
        offset = sum(step * (k >> i & 1) for i, step in enumerate(STEPS))
        block = jnp.bitwise_xor(grp_index, offset)
        for i in range(parts):
            out_ref[block * parts + i, :, 0:width] = share[i * rows : (i + 1) * rows]


def copies_kernel(in_ref, out_ref):
    out_ref[...] = jnp.broadcast_to(in_ref[...][None], out_ref.shape)


def total_kernel(in_ref, out_ref):
    n_tp = in_ref.shape[0]
    total = sum(in_ref[t].astype(F32) for t in range(n_tp)).astype(BF)
    for t in range(n_tp):
        out_ref[t] = total


def finish_kernel(in_ref, out_ref):
    n_tp, rows, _ = in_ref.shape
    parts = out_ref.shape[1] // rows
    blocks = n_tp // parts
    width = out_ref.shape[2] // blocks
    for b in range(blocks):
        for i in range(parts):
            out_ref[0, i * rows : (i + 1) * rows, b * width : (b + 1) * width] = in_ref[
                b * parts + i, :, 0:width
            ].astype(F32)


SMEM = functools.partial(pl.BlockSpec, memory_space=pltpu.SMEM)
VMEM = functools.partial(pl.BlockSpec, memory_space=pltpu.VMEM)
PARAMS = pltpu.CompilerParams(vmem_limit_bytes=16 << 20)


def near(x):
    return x if INTERPRET else pltpu.with_memory_space_constraint(x, pltpu.VMEM)


def far(x):
    return x if INTERPRET else pltpu.with_memory_space_constraint(x, pltpu.HBM)


def near_out(shape, dtype):
    return jax.ShapeDtypeStruct(shape, dtype) if INTERPRET else pltpu.VMEM(shape, dtype)


def copies(piece, count):
    return pl.pallas_call(
        copies_kernel,
        out_shape=near_out((count, *piece.shape), piece.dtype),
        in_specs=[VMEM()],
        out_specs=VMEM(),
        interpret=INTERPRET,
        compiler_params=PARAMS,
        name="copies",
    )(piece)


def attend(info, lens, table, gathered, pool):
    n_tp, slots, _ = gathered.shape
    return pl.pallas_call(
        attend_kernel,
        out_shape=near_out((n_tp, MSG_ROWS, LANES), BF),
        in_specs=[SMEM(), SMEM(), SMEM(), VMEM(), pl.BlockSpec(memory_space=pltpu.HBM)],
        out_specs=VMEM(),
        scratch_shapes=[
            pltpu.VMEM((slots, table.shape[1], *pool.shape[1:]), BF),
            pltpu.VMEM((n_tp * slots, LANES), F32),
            pltpu.VMEM((slots * n_tp, LANES), F32),
            pltpu.VMEM((n_tp, LANES), F32),
            pltpu.SemaphoreType.DMA((slots,)),
        ],
        interpret=INTERPRET,
        compiler_params=PARAMS,
        name="attend",
    )(info, lens, table, near(gathered), far(pool))


def combine(info, message, own, fresh, half, rest):
    n_tp = message.shape[0]
    slots = own.shape[0]
    blocks = 2 ** len(STEPS)
    rows = slots * blocks // n_tp
    width = -(-half.shape[0] * 2 // blocks // LANES) * LANES
    return pl.pallas_call(
        combine_kernel,
        out_shape=near_out((n_tp, rows, width), BF),
        in_specs=[SMEM()] + [VMEM()] * 5,
        out_specs=VMEM(),
        interpret=INTERPRET,
        compiler_params=PARAMS,
        name="combine",
    )(info, near(message), own, fresh, near(half), near(rest))


def total_copies(pieces):
    return pl.pallas_call(
        total_kernel,
        out_shape=near_out(pieces.shape, BF),
        in_specs=[VMEM()],
        out_specs=VMEM(),
        interpret=INTERPRET,
        compiler_params=PARAMS,
        name="total",
    )(near(pieces))


def finish(pieces, slots, width):
    return pl.pallas_call(
        finish_kernel,
        out_shape=jax.ShapeDtypeStruct((1, slots, width), F32),
        in_specs=[VMEM()],
        out_specs=VMEM(),
        interpret=INTERPRET,
        compiler_params=PARAMS,
        name="finish",
    )(near(pieces))


def exchange(pieces, axis):
    return lax.all_to_all(pieces, axis, split_axis=0, concat_axis=0, tiled=True)


def local(batch_sizes, seq_lens, page_table, queries, kv_pool, new_kv, out_weight):
    n_tp = lax.axis_size("tp")
    n_grp = lax.axis_size("grp")
    tp_index = lax.axis_index("tp")
    grp_index = lax.axis_index("grp")
    own = queries[0]
    slots = own.shape[0]
    info = jnp.stack([batch_sizes[0], tp_index.astype(jnp.int32), grp_index.astype(jnp.int32)])

    def from_pair(blocks, step):
        return lax.ppermute(blocks, "grp", [(i, i ^ step) for i in range(n_grp)])

    own_block = out_weight.T
    pair = jnp.concatenate([own_block, from_pair(own_block, STEPS[0])])
    gathered = exchange(copies(own, n_tp), "tp")
    pair, gathered = lax.optimization_barrier((pair, gathered))
    half = jnp.concatenate([pair, from_pair(pair, STEPS[1])])
    message = attend(info, seq_lens[0], page_table[0], gathered, kv_pool[0])
    half, message = lax.optimization_barrier((half, message))
    rest = from_pair(half, STEPS[2])
    received = exchange(message, "tp")
    shares = combine(info, received, own, new_kv[0], half, rest)
    totals = total_copies(exchange(shares, "tp"))
    return finish(exchange(totals, "tp"), slots, n_grp * out_weight.shape[1])


def solution(mesh):
    return jax.shard_map(
        local,
        mesh=mesh,
        in_specs=(
            P("grp"),
            P("grp", None),
            P("grp", None, "tp"),
            P("grp", None, "tp"),
            P("grp", "tp", None, None),
            P("grp", None, None),
            P("tp", "grp"),
        ),
        out_specs=P("grp", None, None),
        check_vma=False,
    )
```

```python
import functools

import jax
import jax.numpy as jnp
from jax import lax
from jax.experimental import pallas as pl
from jax.experimental.pallas import tpu as pltpu
from jax.sharding import PartitionSpec as P


HEADS = 64
KV_HEADS = 8
HD = 64
LANES = 128
NEG_BIG = -1e30
BF = jnp.bfloat16
F32 = jnp.float32
STAT_ROW = 16
MSG_ROWS = 24
INTERPRET = False
STEPS = (4, 1, 2, 3)
UNROLL = 2
AHEAD = 2


def lane_iota(rows):
    return lax.broadcasted_iota(jnp.int32, (rows, LANES), 1)


def roll_lanes(x, shift):
    return pltpu.roll(x, shift, 1)


def split_bf(x):
    hi = x.astype(BF)
    lo = (x - hi.astype(F32)).astype(BF)
    return hi, lo


def attend_kernel(
    info_ref, lens_ref, table_ref, q_ref, pool_ref, out_ref, kv_scr, q_scr, num_scr, stat_scr, sems
):
    n_tp, slots, _ = q_ref.shape
    pages = table_ref.shape[1]
    page_len = pool_ref.shape[1]
    kv_cols = KV_HEADS * HD
    tokens = pages * page_len
    live_count = info_ref[0]
    tp_index = info_ref[1]
    steps = (live_count + UNROLL - 1) // UNROLL

    def load_pages(slot):
        for i in range(pages):
            pltpu.make_async_copy(
                pool_ref.at[table_ref[slot, i]], kv_scr.at[slot, i], sems.at[slot]
            ).start()

    def wait_pages(slot):
        pltpu.make_async_copy(
            pool_ref.at[pl.ds(0, pages)], kv_scr.at[slot], sems.at[slot]
        ).wait()

    for step in range(AHEAD):

        @pl.when(step < steps)
        def _():
            for i in range(UNROLL):
                load_pages(step * UNROLL + i)

    q_scr[...] = (q_ref[...].astype(F32) * HD**-0.5).reshape(n_tp * slots, LANES)
    num_scr[...] = jnp.zeros_like(num_scr)
    low_half = lane_iota(n_tp) < HD
    own_block = (
        lax.broadcasted_iota(jnp.int32, (n_tp, kv_cols), 1) // HD
        == lax.broadcasted_iota(jnp.int32, (n_tp, kv_cols), 0) // (n_tp // KV_HEADS)
    )
    column = lax.broadcasted_iota(jnp.int32, (HEADS, tokens), 1)
    position = (column // page_len) * (page_len * n_tp) + tp_index * page_len + column % page_len
    lane = lane_iota(HEADS)

    def slot_queries(slot):
        x = q_scr[pl.ds(slot, n_tp, stride=slots), :]
        turned = roll_lanes(x, HD)
        even = jnp.where(low_half, x, turned)
        odd = jnp.where(low_half, turned, x)
        wide = [jnp.where(own_block, jnp.concatenate([h] * 4, axis=1), 0.0) for h in (even, odd)]
        return jnp.concatenate(wide, axis=0).astype(BF)

    def slot_scores(slot):
        keys = kv_scr[slot, :, :, 0:kv_cols].reshape(tokens, kv_cols)
        return lax.dot_general(
            slot_queries(slot), keys, (((1,), (1,)), ((), ())), preferred_element_type=F32
        )

    def slot_weights(slot, scores):
        live = position < jnp.where(slot < live_count, lens_ref[slot], 0)
        scores = jnp.where(live, scores, NEG_BIG)
        top = jnp.max(scores, axis=1, keepdims=True)
        top = (top + jnp.abs(top) * 2.0**-7).astype(BF).astype(F32)
        weights = jnp.where(live, jnp.exp(scores - top), 0.0)
        return top, jnp.sum(weights, axis=1, keepdims=True), weights.astype(BF)

    def slot_values(slot, weights):
        values = kv_scr[slot, :, :, kv_cols : 2 * kv_cols].reshape(tokens, kv_cols)
        mixed = jnp.dot(weights, values, preferred_element_type=F32)
        folded = []
        for part in (mixed[:n_tp], mixed[n_tp:]):
            part = jnp.where(own_block, part, 0.0)
            part = sum(part[:, i * LANES : (i + 1) * LANES] for i in range(4))
            folded.append(part + roll_lanes(part, HD))
        num_scr[pl.ds(pl.multiple_of(slot * n_tp, n_tp), n_tp), :] = jnp.where(
            low_half, folded[0], folded[1]
        )

    def some_slots(step, state):
        tops, sums = state
        group = [step * UNROLL + i for i in range(UNROLL)]

        @pl.when(step + AHEAD < steps)
        def _():
            for slot in group:
                load_pages(slot + AHEAD * UNROLL)

        for slot in group:
            wait_pages(slot)
        scores = [slot_scores(slot) for slot in group]
        parts = [slot_weights(slot, s) for slot, s in zip(group, scores)]
        for slot, (top, total, weights) in zip(group, parts):
            slot_values(slot, weights)
            here = lane == slot
            tops = jnp.where(here, top, tops)
            sums = jnp.where(here, total, sums)
        return tops, sums

    start = (
        jnp.where(lane < slots, NEG_BIG, 0.0).astype(F32),
        jnp.zeros((HEADS, LANES), F32),
    )
    tops, sums = lax.fori_loop(0, steps, some_slots, start)
    hi, lo = split_bf(sums)
    packed = tops + roll_lanes(hi.astype(F32), slots) + roll_lanes(lo.astype(F32), 2 * slots)
    stat_scr[...] = packed[:n_tp] + roll_lanes(packed[n_tp:], HD)
    for t in range(n_tp):
        out_ref[t, 0:slots, :] = num_scr[pl.ds(t, slots, stride=n_tp), :].astype(BF)
        out_ref[t, STAT_ROW:MSG_ROWS, :] = jnp.broadcast_to(
            stat_scr[t : t + 1, :], (MSG_ROWS - STAT_ROW, LANES)
        ).astype(BF)


def combine_kernel(info_ref, msg_ref, q_ref, new_ref, *rest):
    pair_refs, out_ref = rest[:-1], rest[-1]
    n_tp = msg_ref.shape[0]
    slots = q_ref.shape[0]
    live_count = info_ref[0]
    tp_index = info_ref[1]
    grp_index = info_ref[2]
    blocks = 2 * len(pair_refs)
    width = pair_refs[0].shape[0] // 2
    ones_block = (
        lax.broadcasted_iota(jnp.int32, (LANES, LANES), 0) // HD
        == lax.broadcasted_iota(jnp.int32, (LANES, LANES), 1) // HD
    ).astype(F32).astype(BF)
    rows8 = MSG_ROWS - STAT_ROW
    stats = [msg_ref[t, STAT_ROW:MSG_ROWS, :].astype(F32) for t in range(n_tp)]
    top = functools.reduce(jnp.maximum, stats)
    scale = [jnp.exp(s - top) for s in stats]
    sums = sum(
        w * (roll_lanes(s, LANES - slots) + roll_lanes(s, LANES - 2 * slots))
        for w, s in zip(scale, stats)
    )
    sub = lax.broadcasted_iota(jnp.int32, (rows8, LANES), 0)
    within = lane_iota(rows8) % HD
    picks = [within == sub + rows8 * i for i in range(slots // rows8)]
    picked = jnp.concatenate(
        [jnp.where(p, v, 0.0) for v in (*scale, top, sums) for p in picks], axis=0
    )
    hi, lo = split_bf(picked)
    spread = jnp.dot(hi, ones_block, preferred_element_type=F32) + jnp.dot(
        lo, ones_block, preferred_element_type=F32
    )
    top_all = spread[n_tp * slots : (n_tp + 1) * slots]
    sum_all = spread[(n_tp + 1) * slots :]
    numerator = sum(
        msg_ref[t, 0:slots, :].astype(F32) * spread[t * slots : (t + 1) * slots]
        for t in range(n_tp)
    )

    kv_head = tp_index // (n_tp // KV_HEADS)
    low_half = lane_iota(slots) < HD

    def own_columns(first):
        at = pl.multiple_of(first + (kv_head // 2) * LANES, LANES)
        block = new_ref[:, pl.ds(at, LANES)].astype(F32)
        turned = roll_lanes(block, HD)
        low = jnp.where(low_half, block, turned)
        high = jnp.where(low_half, turned, block)
        return jnp.where(kv_head % 2 == 0, low, high)

    new_key = own_columns(0)
    new_value = own_columns(KV_HEADS * HD)
    products = q_ref[...].astype(F32) * HD**-0.5 * new_key
    hi, lo = split_bf(products)
    self_score = jnp.dot(hi, ones_block, preferred_element_type=F32) + jnp.dot(
        lo, ones_block, preferred_element_type=F32
    )
    final_top = jnp.maximum(top_all, self_score)
    cached = jnp.exp(top_all - final_top)
    fresh = jnp.exp(self_score - final_top)
    attended = (numerator * cached + new_value * fresh) / (sum_all * cached + fresh)
    slot = lax.broadcasted_iota(jnp.int32, (slots, LANES), 0)
    attended = jnp.where(slot < live_count, attended, 0.0).astype(BF)
    parts = n_tp // blocks
    rows = slots // parts
    for k in range(blocks):
        first = k % 2 * width
        share = lax.dot_general(
            attended,
            pair_refs[k // 2][first : first + width, :],
            (((1,), (1,)), ((), ())),
            preferred_element_type=F32,
        ).astype(BF)
        offset = (0, STEPS[0])[k % 2] ^ (0, *STEPS[1:])[k // 2]
        block = jnp.bitwise_xor(grp_index, offset)
        for i in range(parts):
            out_ref[block * parts + i, :, 0:width] = share[i * rows : (i + 1) * rows]


def copies_kernel(in_ref, out_ref):
    out_ref[...] = jnp.broadcast_to(in_ref[...][None], out_ref.shape)


def total_kernel(in_ref, out_ref):
    n_tp = in_ref.shape[0]
    total = sum(in_ref[t].astype(F32) for t in range(n_tp)).astype(BF)
    for t in range(n_tp):
        out_ref[t] = total


def finish_kernel(in_ref, out_ref):
    n_tp, rows, _ = in_ref.shape
    parts = out_ref.shape[1] // rows
    blocks = n_tp // parts
    width = out_ref.shape[2] // blocks
    for b in range(blocks):
        for i in range(parts):
            out_ref[0, i * rows : (i + 1) * rows, b * width : (b + 1) * width] = in_ref[
                b * parts + i, :, 0:width
            ].astype(F32)


SMEM = functools.partial(pl.BlockSpec, memory_space=pltpu.SMEM)
VMEM = functools.partial(pl.BlockSpec, memory_space=pltpu.VMEM)
PARAMS = pltpu.CompilerParams(vmem_limit_bytes=16 << 20)


def near(x):
    return x if INTERPRET else pltpu.with_memory_space_constraint(x, pltpu.VMEM)


def far(x):
    return x if INTERPRET else pltpu.with_memory_space_constraint(x, pltpu.HBM)


def near_out(shape, dtype):
    return jax.ShapeDtypeStruct(shape, dtype) if INTERPRET else pltpu.VMEM(shape, dtype)


def copies(piece, count):
    return pl.pallas_call(
        copies_kernel,
        out_shape=near_out((count, *piece.shape), piece.dtype),
        in_specs=[VMEM()],
        out_specs=VMEM(),
        interpret=INTERPRET,
        compiler_params=PARAMS,
        name="copies",
    )(far(piece))


def attend(info, lens, table, gathered, pool):
    n_tp, slots, _ = gathered.shape
    return pl.pallas_call(
        attend_kernel,
        out_shape=near_out((n_tp, MSG_ROWS, LANES), BF),
        in_specs=[SMEM(), SMEM(), SMEM(), VMEM(), pl.BlockSpec(memory_space=pltpu.HBM)],
        out_specs=VMEM(),
        scratch_shapes=[
            pltpu.VMEM((slots, table.shape[1], *pool.shape[1:]), BF),
            pltpu.VMEM((n_tp * slots, LANES), F32),
            pltpu.VMEM((slots * n_tp, LANES), F32),
            pltpu.VMEM((n_tp, LANES), F32),
            pltpu.SemaphoreType.DMA((slots,)),
        ],
        interpret=INTERPRET,
        compiler_params=PARAMS,
        name="attend",
    )(info, far(lens), far(table), near(gathered), far(pool))


def combine(info, message, own, fresh, pairs):
    n_tp = message.shape[0]
    slots = own.shape[0]
    rows = slots * 2 * len(pairs) // n_tp
    width = -(-pairs[0].shape[0] // 2 // LANES) * LANES
    return pl.pallas_call(
        combine_kernel,
        out_shape=near_out((n_tp, rows, width), BF),
        in_specs=[SMEM()] + [VMEM()] * (3 + len(pairs)),
        out_specs=VMEM(),
        interpret=INTERPRET,
        compiler_params=PARAMS,
        name="combine",
    )(info, near(message), near(own), near(fresh), *map(near, pairs))


def total_copies(pieces):
    return pl.pallas_call(
        total_kernel,
        out_shape=near_out(pieces.shape, BF),
        in_specs=[VMEM()],
        out_specs=VMEM(),
        interpret=INTERPRET,
        compiler_params=PARAMS,
        name="total",
    )(near(pieces))


def finish(pieces, slots, width):
    return pl.pallas_call(
        finish_kernel,
        out_shape=jax.ShapeDtypeStruct((1, slots, width), F32),
        in_specs=[VMEM()],
        out_specs=VMEM(),
        interpret=INTERPRET,
        compiler_params=PARAMS,
        name="finish",
    )(near(pieces))


def exchange(pieces, axis):
    return lax.all_to_all(pieces, axis, split_axis=0, concat_axis=0, tiled=True)


def local(batch_sizes, seq_lens, page_table, queries, kv_pool, new_kv, out_weight):
    n_tp = lax.axis_size("tp")
    n_grp = lax.axis_size("grp")
    tp_index = lax.axis_index("tp")
    grp_index = lax.axis_index("grp")
    own = queries[0]
    slots = own.shape[0]
    info = jnp.stack([batch_sizes[0], tp_index.astype(jnp.int32), grp_index.astype(jnp.int32)])

    def from_pair(blocks, step):
        return lax.ppermute(blocks, "grp", [(i, i ^ step) for i in range(n_grp)])

    own_block = out_weight.T
    pair = jnp.concatenate([own_block, from_pair(own_block, STEPS[0])])
    gathered = exchange(copies(own, n_tp), "tp")
    pair, gathered = lax.optimization_barrier((pair, gathered))
    pairs = [pair] + [from_pair(pair, step) for step in STEPS[1:]]
    message = attend(info, seq_lens[0], page_table[0], gathered, kv_pool[0])
    received = exchange(message, "tp")
    shares = combine(info, received, own, new_kv[0], pairs)
    totals = total_copies(exchange(shares, "tp"))
    return finish(exchange(totals, "tp"), slots, n_grp * out_weight.shape[1])


def solution(mesh):
    return jax.shard_map(
        local,
        mesh=mesh,
        in_specs=(
            P("grp"),
            P("grp", None),
            P("grp", None, "tp"),
            P("grp", None, "tp"),
            P("grp", "tp", None, None),
            P("grp", None, None),
            P("tp", "grp"),
        ),
        out_specs=P("grp", None, None),
        check_vma=False,
    )
```

```python
import functools

import jax
import jax.numpy as jnp
from jax import lax
from jax.experimental import pallas as pl
from jax.experimental.pallas import tpu as pltpu
from jax.sharding import PartitionSpec as P


HEADS = 64
KV_HEADS = 8
HD = 64
LANES = 128
NEG_BIG = -1e30
BF = jnp.bfloat16
F32 = jnp.float32
STAT_ROW = 16
MSG_ROWS = 24
INTERPRET = False
EARLY = (6, 7, 5, 2)
LATE = (1, 3, 4)
UNROLL = 2
CHUNK = 4


def axis_index(name):
    return INTERPRET[name] if INTERPRET else lax.axis_index(name)


def lane_iota(rows):
    return lax.broadcasted_iota(jnp.int32, (rows, LANES), 1)


def roll_lanes(x, shift):
    return pltpu.roll(x, shift, 1)


def split_bf(x):
    hi = x.astype(BF)
    lo = (x - hi.astype(F32)).astype(BF)
    return hi, lo


def attend_kernel(
    size_ref, lens_ref, table_ref, q_ref, pool_ref, out_ref, kv_scr, q_scr, num_scr, stat_scr, sems
):
    n_tp, slots, _ = q_ref.shape
    pages = table_ref.shape[1]
    page_len = pool_ref.shape[1]
    kv_cols = KV_HEADS * HD
    tokens = pages * page_len
    live_count = size_ref[0]
    tp_index = axis_index("tp")
    steps = (live_count + UNROLL - 1) // UNROLL

    def live_length(slot):
        return jnp.where(slot < live_count, lens_ref[slot], 0)

    def is_live(slot, chunk):
        first_page = chunk * CHUNK
        return (first_page * n_tp + tp_index) * page_len < live_length(slot)

    def load_pages(slot):
        for chunk in range(pages // CHUNK):

            @pl.when(is_live(slot, chunk))
            def _():
                for i in range(chunk * CHUNK, (chunk + 1) * CHUNK):
                    pltpu.make_async_copy(
                        pool_ref.at[table_ref[slot, i]],
                        kv_scr.at[slot, i],
                        sems.at[slot, chunk],
                    ).start()

            @pl.when(jnp.logical_not(is_live(slot, chunk)))
            def _():
                kv_scr[slot, chunk * CHUNK : (chunk + 1) * CHUNK, :, kv_cols:] = jnp.zeros(
                    (CHUNK, page_len, kv_cols), BF
                )

    def wait_pages(slot):
        for chunk in range(pages // CHUNK):

            @pl.when(is_live(slot, chunk))
            def _():
                pltpu.make_async_copy(
                    pool_ref.at[pl.ds(0, CHUNK)],
                    kv_scr.at[slot, pl.ds(chunk * CHUNK, CHUNK)],
                    sems.at[slot, chunk],
                ).wait()

    lax.fori_loop(0, steps * UNROLL, lambda slot, _: load_pages(slot), None)
    q_scr[...] = (q_ref[...].astype(F32) * HD**-0.5).reshape(n_tp * slots, LANES)
    num_scr[...] = jnp.zeros_like(num_scr)
    low_half = lane_iota(n_tp) < HD
    own_block = (
        lax.broadcasted_iota(jnp.int32, (n_tp, kv_cols), 1) // HD
        == lax.broadcasted_iota(jnp.int32, (n_tp, kv_cols), 0) // (n_tp // KV_HEADS)
    )
    column = lax.broadcasted_iota(jnp.int32, (HEADS, tokens), 1)
    position = (column // page_len) * (page_len * n_tp) + tp_index * page_len + column % page_len
    lane = lane_iota(HEADS)

    def slot_queries(slot):
        x = q_scr[pl.ds(slot, n_tp, stride=slots), :]
        turned = roll_lanes(x, HD)
        even = jnp.where(low_half, x, turned)
        odd = jnp.where(low_half, turned, x)
        wide = [jnp.where(own_block, jnp.concatenate([h] * 4, axis=1), 0.0) for h in (even, odd)]
        return jnp.concatenate(wide, axis=0).astype(BF)

    def slot_scores(slot):
        keys = kv_scr[slot, :, :, 0:kv_cols].reshape(tokens, kv_cols)
        return lax.dot_general(
            slot_queries(slot), keys, (((1,), (1,)), ((), ())), preferred_element_type=F32
        )

    def slot_weights(slot, scores):
        live = position < live_length(slot)
        scores = jnp.where(live, scores, NEG_BIG)
        top = jnp.max(scores, axis=1, keepdims=True)
        top = (top + jnp.abs(top) * 2.0**-7).astype(BF).astype(F32)
        weights = jnp.where(live, jnp.exp(scores - top), 0.0)
        return top, jnp.sum(weights, axis=1, keepdims=True), weights.astype(BF)

    def slot_values(slot, weights):
        values = kv_scr[slot, :, :, kv_cols : 2 * kv_cols].reshape(tokens, kv_cols)
        mixed = jnp.dot(weights, values, preferred_element_type=F32)
        folded = []
        for part in (mixed[:n_tp], mixed[n_tp:]):
            part = jnp.where(own_block, part, 0.0)
            part = sum(part[:, i * LANES : (i + 1) * LANES] for i in range(4))
            folded.append(part + roll_lanes(part, HD))
        num_scr[pl.ds(pl.multiple_of(slot * n_tp, n_tp), n_tp), :] = jnp.where(
            low_half, folded[0], folded[1]
        )

    def some_slots(step, state):
        tops, sums = state
        group = [step * UNROLL + i for i in range(UNROLL)]
        for slot in group:
            wait_pages(slot)
        scores = [slot_scores(slot) for slot in group]
        parts = [slot_weights(slot, s) for slot, s in zip(group, scores)]
        for slot, (top, total, weights) in zip(group, parts):
            slot_values(slot, weights)
            here = lane == slot
            tops = jnp.where(here, top, tops)
            sums = jnp.where(here, total, sums)
        return tops, sums

    start = (
        jnp.where(lane < slots, NEG_BIG, 0.0).astype(F32),
        jnp.zeros((HEADS, LANES), F32),
    )
    tops, sums = lax.fori_loop(0, steps, some_slots, start)
    hi, lo = split_bf(sums)
    packed = tops + roll_lanes(hi.astype(F32), slots) + roll_lanes(lo.astype(F32), 2 * slots)
    stat_scr[...] = packed[:n_tp] + roll_lanes(packed[n_tp:], HD)
    for t in range(n_tp):
        out_ref[t, 0:slots, :] = num_scr[pl.ds(t, slots, stride=n_tp), :].astype(BF)
        out_ref[t, STAT_ROW:MSG_ROWS, :] = jnp.broadcast_to(
            stat_scr[t : t + 1, :], (MSG_ROWS - STAT_ROW, LANES)
        ).astype(BF)


def combine_kernel(offsets, size_ref, msg_ref, q_ref, new_ref, *rest):
    block_refs, out_ref = rest[:-1], rest[-1]
    n_tp = msg_ref.shape[0]
    slots = q_ref.shape[0]
    live_count = size_ref[0]
    tp_index = axis_index("tp")
    grp_index = axis_index("grp")
    blocks = len(block_refs)
    width = block_refs[0].shape[0]
    ones_block = (
        lax.broadcasted_iota(jnp.int32, (LANES, LANES), 0) // HD
        == lax.broadcasted_iota(jnp.int32, (LANES, LANES), 1) // HD
    ).astype(F32).astype(BF)
    rows8 = MSG_ROWS - STAT_ROW
    stats = [msg_ref[t, STAT_ROW:MSG_ROWS, :].astype(F32) for t in range(n_tp)]
    top = functools.reduce(jnp.maximum, stats)
    scale = [jnp.exp(s - top) for s in stats]
    sums = sum(
        w * (roll_lanes(s, LANES - slots) + roll_lanes(s, LANES - 2 * slots))
        for w, s in zip(scale, stats)
    )
    sub = lax.broadcasted_iota(jnp.int32, (rows8, LANES), 0)
    within = lane_iota(rows8) % HD
    picks = [within == sub + rows8 * i for i in range(slots // rows8)]
    picked = jnp.concatenate(
        [jnp.where(p, v, 0.0) for v in (*scale, top, sums) for p in picks], axis=0
    )
    hi, lo = split_bf(picked)
    spread = jnp.dot(hi, ones_block, preferred_element_type=F32) + jnp.dot(
        lo, ones_block, preferred_element_type=F32
    )
    top_all = spread[n_tp * slots : (n_tp + 1) * slots]
    sum_all = spread[(n_tp + 1) * slots :]
    numerator = sum(
        msg_ref[t, 0:slots, :].astype(F32) * spread[t * slots : (t + 1) * slots]
        for t in range(n_tp)
    )

    kv_head = tp_index // (n_tp // KV_HEADS)
    low_half = lane_iota(slots) < HD

    def own_columns(first):
        at = pl.multiple_of(first + (kv_head // 2) * LANES, LANES)
        block = new_ref[:, pl.ds(at, LANES)].astype(F32)
        turned = roll_lanes(block, HD)
        low = jnp.where(low_half, block, turned)
        high = jnp.where(low_half, turned, block)
        return jnp.where(kv_head % 2 == 0, low, high)

    new_key = own_columns(0)
    new_value = own_columns(KV_HEADS * HD)
    products = q_ref[...].astype(F32) * HD**-0.5 * new_key
    hi, lo = split_bf(products)
    self_score = jnp.dot(hi, ones_block, preferred_element_type=F32) + jnp.dot(
        lo, ones_block, preferred_element_type=F32
    )
    final_top = jnp.maximum(top_all, self_score)
    cached = jnp.exp(top_all - final_top)
    fresh = jnp.exp(self_score - final_top)
    attended = (numerator * cached + new_value * fresh) / (sum_all * cached + fresh)
    slot = lax.broadcasted_iota(jnp.int32, (slots, LANES), 0)
    attended = jnp.where(slot < live_count, attended, 0.0).astype(BF)
    parts = n_tp // blocks
    rows = slots // parts
    for offset, block_ref in zip(offsets, block_refs):
        share = lax.dot_general(
            attended, block_ref[...], (((1,), (1,)), ((), ())), preferred_element_type=F32
        ).astype(BF)
        block = jnp.bitwise_xor(grp_index, offset)
        for i in range(parts):
            out_ref[block * parts + i, :, 0:width] = share[i * rows : (i + 1) * rows]


def copies_kernel(in_ref, out_ref):
    out_ref[...] = jnp.broadcast_to(in_ref[...][None], out_ref.shape)


def total_kernel(in_ref, out_ref):
    n_tp = in_ref.shape[0]
    total = sum(in_ref[t].astype(F32) for t in range(n_tp)).astype(BF)
    for t in range(n_tp):
        out_ref[t] = total


def finish_kernel(in_ref, out_ref):
    n_tp, rows, _ = in_ref.shape
    parts = out_ref.shape[1] // rows
    blocks = n_tp // parts
    width = out_ref.shape[2] // blocks
    for b in range(blocks):
        for i in range(parts):
            out_ref[0, i * rows : (i + 1) * rows, b * width : (b + 1) * width] = in_ref[
                b * parts + i, :, 0:width
            ].astype(F32)


SMEM = functools.partial(pl.BlockSpec, memory_space=pltpu.SMEM)
VMEM = functools.partial(pl.BlockSpec, memory_space=pltpu.VMEM)
PARAMS = pltpu.CompilerParams(vmem_limit_bytes=16 << 20)


def near(x):
    return x if INTERPRET else pltpu.with_memory_space_constraint(x, pltpu.VMEM)


def far(x):
    return x if INTERPRET else pltpu.with_memory_space_constraint(x, pltpu.HBM)


def near_out(shape, dtype):
    return jax.ShapeDtypeStruct(shape, dtype) if INTERPRET else pltpu.VMEM(shape, dtype)


def copies(piece, count):
    return pl.pallas_call(
        copies_kernel,
        out_shape=near_out((count, *piece.shape), piece.dtype),
        in_specs=[VMEM()],
        out_specs=VMEM(),
        interpret=bool(INTERPRET),
        compiler_params=PARAMS,
        name="copies",
    )(far(piece))


def attend(sizes, lens, table, gathered, pool):
    n_tp, slots, _ = gathered.shape
    return pl.pallas_call(
        attend_kernel,
        out_shape=near_out((n_tp, MSG_ROWS, LANES), BF),
        in_specs=[SMEM(), SMEM(), SMEM(), VMEM(), pl.BlockSpec(memory_space=pltpu.HBM)],
        out_specs=VMEM(),
        scratch_shapes=[
            pltpu.VMEM((slots, table.shape[1], *pool.shape[1:]), BF),
            pltpu.VMEM((n_tp * slots, LANES), F32),
            pltpu.VMEM((slots * n_tp, LANES), F32),
            pltpu.VMEM((n_tp, LANES), F32),
            pltpu.SemaphoreType.DMA((slots, table.shape[1] // CHUNK)),
        ],
        interpret=bool(INTERPRET),
        compiler_params=PARAMS,
        name="attend",
    )(sizes, far(lens), far(table), near(gathered), far(pool))


def combine(sizes, message, own, fresh, blocks):
    n_tp = message.shape[0]
    slots = own.shape[0]
    rows = slots * len(blocks) // n_tp
    width = -(-blocks[0].shape[0] // LANES) * LANES
    return pl.pallas_call(
        functools.partial(combine_kernel, tuple(blocks)),
        out_shape=near_out((n_tp, rows, width), BF),
        in_specs=[SMEM()] + [VMEM()] * (3 + len(blocks)),
        out_specs=VMEM(),
        interpret=bool(INTERPRET),
        compiler_params=PARAMS,
        name="combine",
    )(sizes, near(message), near(own), near(fresh), *map(near, blocks.values()))


def total_copies(pieces):
    return pl.pallas_call(
        total_kernel,
        out_shape=near_out(pieces.shape, BF),
        in_specs=[VMEM()],
        out_specs=VMEM(),
        interpret=bool(INTERPRET),
        compiler_params=PARAMS,
        name="total",
    )(near(pieces))


def finish(pieces, slots, width):
    return pl.pallas_call(
        finish_kernel,
        out_shape=jax.ShapeDtypeStruct((1, slots, width), F32),
        in_specs=[VMEM()],
        out_specs=VMEM(),
        interpret=bool(INTERPRET),
        compiler_params=PARAMS,
        name="finish",
    )(near(pieces))


def exchange(pieces, axis):
    return lax.all_to_all(pieces, axis, split_axis=0, concat_axis=0, tiled=True)


def local(batch_sizes, seq_lens, page_table, queries, kv_pool, new_kv, out_weight):
    n_tp = lax.axis_size("tp")
    n_grp = lax.axis_size("grp")
    own = queries[0]
    slots = own.shape[0]

    def from_pair(block, step):
        return lax.ppermute(block, "grp", [(i, i ^ step) for i in range(n_grp)])

    own_block = out_weight.T
    blocks = {0: own_block}
    for step in EARLY:
        blocks[step] = from_pair(own_block, step)
    gathered = exchange(copies(own, n_tp), "tp")
    message = attend(batch_sizes, seq_lens[0], page_table[0], gathered, kv_pool[0])
    late_block, message = lax.optimization_barrier((own_block, message))
    for step in LATE:
        blocks[step] = from_pair(late_block, step)
    received = exchange(message, "tp")
    shares = combine(batch_sizes, received, own, new_kv[0], blocks)
    totals = total_copies(exchange(shares, "tp"))
    return finish(exchange(totals, "tp"), slots, n_grp * out_weight.shape[1])


def solution(mesh):
    return jax.shard_map(
        local,
        mesh=mesh,
        in_specs=(
            P("grp"),
            P("grp", None),
            P("grp", None, "tp"),
            P("grp", None, "tp"),
            P("grp", "tp", None, None),
            P("grp", None, None),
            P("tp", "grp"),
        ),
        out_specs=P("grp", None, None),
        check_vma=False,
    )
```

```python
import functools

import jax
import jax.numpy as jnp
from jax import lax
from jax.experimental import pallas as pl
from jax.experimental.pallas import tpu as pltpu
from jax.sharding import PartitionSpec as P


HEADS = 64
KV_HEADS = 8
HD = 64
LANES = 128
NEG_BIG = -1e30
BF = jnp.bfloat16
F32 = jnp.float32
STAT_ROW = 16
MSG_ROWS = 24
INTERPRET = False
FIRST_STEP = 4
PAIR_STEPS = (2, 3, 1)
UNROLL = 2
CHUNK = 4


def axis_index(name):
    return INTERPRET[name] if INTERPRET else lax.axis_index(name)


def lane_iota(rows):
    return lax.broadcasted_iota(jnp.int32, (rows, LANES), 1)


def roll_lanes(x, shift):
    return pltpu.roll(x, shift, 1)


def split_bf(x):
    hi = x.astype(BF)
    lo = (x - hi.astype(F32)).astype(BF)
    return hi, lo


def attend_kernel(
    size_ref, lens_ref, table_ref, q_ref, pool_ref, out_ref, kv_scr, q_scr, num_scr, stat_scr, sems
):
    n_tp, slots, _ = q_ref.shape
    pages = table_ref.shape[1]
    page_len = pool_ref.shape[1]
    kv_cols = KV_HEADS * HD
    tokens = pages * page_len
    live_count = size_ref[0]
    tp_index = axis_index("tp")
    steps = (live_count + UNROLL - 1) // UNROLL

    def live_length(slot):
        return jnp.where(slot < live_count, lens_ref[slot], 0)

    def is_live(slot, chunk):
        first_page = chunk * CHUNK
        return (first_page * n_tp + tp_index) * page_len < live_length(slot)

    def load_pages(slot):
        for chunk in range(pages // CHUNK):

            @pl.when(is_live(slot, chunk))
            def _():
                for i in range(chunk * CHUNK, (chunk + 1) * CHUNK):
                    pltpu.make_async_copy(
                        pool_ref.at[table_ref[slot, i]],
                        kv_scr.at[slot, i],
                        sems.at[slot, chunk],
                    ).start()

            @pl.when(jnp.logical_not(is_live(slot, chunk)))
            def _():
                kv_scr[slot, chunk * CHUNK : (chunk + 1) * CHUNK, :, kv_cols:] = jnp.zeros(
                    (CHUNK, page_len, kv_cols), BF
                )

    def wait_pages(slot):
        for chunk in range(pages // CHUNK):

            @pl.when(is_live(slot, chunk))
            def _():
                pltpu.make_async_copy(
                    pool_ref.at[pl.ds(0, CHUNK)],
                    kv_scr.at[slot, pl.ds(chunk * CHUNK, CHUNK)],
                    sems.at[slot, chunk],
                ).wait()

    lax.fori_loop(0, steps * UNROLL, lambda slot, _: load_pages(slot), None)
    q_scr[...] = (q_ref[...].astype(F32) * HD**-0.5).reshape(n_tp * slots, LANES)
    num_scr[...] = jnp.zeros_like(num_scr)
    low_half = lane_iota(n_tp) < HD
    own_block = (
        lax.broadcasted_iota(jnp.int32, (n_tp, kv_cols), 1) // HD
        == lax.broadcasted_iota(jnp.int32, (n_tp, kv_cols), 0) // (n_tp // KV_HEADS)
    )
    column = lax.broadcasted_iota(jnp.int32, (HEADS, tokens), 1)
    position = (column // page_len) * (page_len * n_tp) + tp_index * page_len + column % page_len
    lane = lane_iota(HEADS)

    def slot_queries(slot):
        x = q_scr[pl.ds(slot, n_tp, stride=slots), :]
        turned = roll_lanes(x, HD)
        even = jnp.where(low_half, x, turned)
        odd = jnp.where(low_half, turned, x)
        wide = [jnp.where(own_block, jnp.concatenate([h] * 4, axis=1), 0.0) for h in (even, odd)]
        return jnp.concatenate(wide, axis=0).astype(BF)

    def slot_scores(slot):
        keys = kv_scr[slot, :, :, 0:kv_cols].reshape(tokens, kv_cols)
        return lax.dot_general(
            slot_queries(slot), keys, (((1,), (1,)), ((), ())), preferred_element_type=F32
        )

    def slot_weights(slot, scores):
        live = position < live_length(slot)
        scores = jnp.where(live, scores, NEG_BIG)
        top = jnp.max(scores, axis=1, keepdims=True)
        top = (top + jnp.abs(top) * 2.0**-7).astype(BF).astype(F32)
        weights = jnp.where(live, jnp.exp(scores - top), 0.0)
        return top, jnp.sum(weights, axis=1, keepdims=True), weights.astype(BF)

    def slot_values(slot, weights):
        values = kv_scr[slot, :, :, kv_cols : 2 * kv_cols].reshape(tokens, kv_cols)
        mixed = jnp.dot(weights, values, preferred_element_type=F32)
        folded = []
        for part in (mixed[:n_tp], mixed[n_tp:]):
            part = jnp.where(own_block, part, 0.0)
            part = sum(part[:, i * LANES : (i + 1) * LANES] for i in range(4))
            folded.append(part + roll_lanes(part, HD))
        num_scr[pl.ds(pl.multiple_of(slot * n_tp, n_tp), n_tp), :] = jnp.where(
            low_half, folded[0], folded[1]
        )

    def some_slots(step, state):
        tops, sums = state
        group = [step * UNROLL + i for i in range(UNROLL)]
        for slot in group:
            wait_pages(slot)
        scores = [slot_scores(slot) for slot in group]
        parts = [slot_weights(slot, s) for slot, s in zip(group, scores)]
        for slot, (top, total, weights) in zip(group, parts):
            slot_values(slot, weights)
            here = lane == slot
            tops = jnp.where(here, top, tops)
            sums = jnp.where(here, total, sums)
        return tops, sums

    start = (
        jnp.where(lane < slots, NEG_BIG, 0.0).astype(F32),
        jnp.zeros((HEADS, LANES), F32),
    )
    tops, sums = lax.fori_loop(0, steps, some_slots, start)
    hi, lo = split_bf(sums)
    packed = tops + roll_lanes(hi.astype(F32), slots) + roll_lanes(lo.astype(F32), 2 * slots)
    stat_scr[...] = packed[:n_tp] + roll_lanes(packed[n_tp:], HD)
    for t in range(n_tp):
        out_ref[t, 0:slots, :] = num_scr[pl.ds(t, slots, stride=n_tp), :].astype(BF)
        out_ref[t, STAT_ROW:MSG_ROWS, :] = jnp.broadcast_to(
            stat_scr[t : t + 1, :], (MSG_ROWS - STAT_ROW, LANES)
        ).astype(BF)


def combine_kernel(offsets, size_ref, msg_ref, q_ref, new_ref, *rest):
    pair_refs, out_ref = rest[:-1], rest[-1]
    n_tp = msg_ref.shape[0]
    slots = q_ref.shape[0]
    live_count = size_ref[0]
    tp_index = axis_index("tp")
    grp_index = axis_index("grp")
    blocks = 2 * len(pair_refs)
    width = pair_refs[0].shape[0] // 2
    ones_block = (
        lax.broadcasted_iota(jnp.int32, (LANES, LANES), 0) // HD
        == lax.broadcasted_iota(jnp.int32, (LANES, LANES), 1) // HD
    ).astype(F32).astype(BF)
    rows8 = MSG_ROWS - STAT_ROW
    stats = [msg_ref[t, STAT_ROW:MSG_ROWS, :].astype(F32) for t in range(n_tp)]
    top = functools.reduce(jnp.maximum, stats)
    scale = [jnp.exp(s - top) for s in stats]
    sums = sum(
        w * (roll_lanes(s, LANES - slots) + roll_lanes(s, LANES - 2 * slots))
        for w, s in zip(scale, stats)
    )
    sub = lax.broadcasted_iota(jnp.int32, (rows8, LANES), 0)
    within = lane_iota(rows8) % HD
    picks = [within == sub + rows8 * i for i in range(slots // rows8)]
    picked = jnp.concatenate(
        [jnp.where(p, v, 0.0) for v in (*scale, top, sums) for p in picks], axis=0
    )
    hi, lo = split_bf(picked)
    spread = jnp.dot(hi, ones_block, preferred_element_type=F32) + jnp.dot(
        lo, ones_block, preferred_element_type=F32
    )
    top_all = spread[n_tp * slots : (n_tp + 1) * slots]
    sum_all = spread[(n_tp + 1) * slots :]
    numerator = sum(
        msg_ref[t, 0:slots, :].astype(F32) * spread[t * slots : (t + 1) * slots]
        for t in range(n_tp)
    )

    kv_head = tp_index // (n_tp // KV_HEADS)
    low_half = lane_iota(slots) < HD

    def own_columns(first):
        at = pl.multiple_of(first + (kv_head // 2) * LANES, LANES)
        block = new_ref[:, pl.ds(at, LANES)].astype(F32)
        turned = roll_lanes(block, HD)
        low = jnp.where(low_half, block, turned)
        high = jnp.where(low_half, turned, block)
        return jnp.where(kv_head % 2 == 0, low, high)

    new_key = own_columns(0)
    new_value = own_columns(KV_HEADS * HD)
    products = q_ref[...].astype(F32) * HD**-0.5 * new_key
    hi, lo = split_bf(products)
    self_score = jnp.dot(hi, ones_block, preferred_element_type=F32) + jnp.dot(
        lo, ones_block, preferred_element_type=F32
    )
    final_top = jnp.maximum(top_all, self_score)
    cached = jnp.exp(top_all - final_top)
    fresh = jnp.exp(self_score - final_top)
    attended = (numerator * cached + new_value * fresh) / (sum_all * cached + fresh)
    slot = lax.broadcasted_iota(jnp.int32, (slots, LANES), 0)
    attended = jnp.where(slot < live_count, attended, 0.0).astype(BF)
    parts = n_tp // blocks
    rows = slots // parts
    for offset, pair_ref in zip(offsets, pair_refs):
        for half in range(2):
            share = lax.dot_general(
                attended,
                pair_ref[half * width : (half + 1) * width, :],
                (((1,), (1,)), ((), ())),
                preferred_element_type=F32,
            ).astype(BF)
            block = jnp.bitwise_xor(grp_index, offset ^ (half * FIRST_STEP))
            for i in range(parts):
                out_ref[block * parts + i, :, 0:width] = share[i * rows : (i + 1) * rows]


def copies_kernel(in_ref, out_ref):
    out_ref[...] = jnp.broadcast_to(in_ref[...][None], out_ref.shape)


def total_kernel(in_ref, out_ref):
    n_tp = in_ref.shape[0]
    total = sum(in_ref[t].astype(F32) for t in range(n_tp)).astype(BF)
    for t in range(n_tp):
        out_ref[t] = total


def finish_kernel(in_ref, out_ref):
    n_tp, rows, _ = in_ref.shape
    parts = out_ref.shape[1] // rows
    blocks = n_tp // parts
    width = out_ref.shape[2] // blocks
    for b in range(blocks):
        for i in range(parts):
            out_ref[0, i * rows : (i + 1) * rows, b * width : (b + 1) * width] = in_ref[
                b * parts + i, :, 0:width
            ].astype(F32)


SMEM = functools.partial(pl.BlockSpec, memory_space=pltpu.SMEM)
VMEM = functools.partial(pl.BlockSpec, memory_space=pltpu.VMEM)
PARAMS = pltpu.CompilerParams(vmem_limit_bytes=16 << 20)


def near(x):
    return x if INTERPRET else pltpu.with_memory_space_constraint(x, pltpu.VMEM)


def far(x):
    return x if INTERPRET else pltpu.with_memory_space_constraint(x, pltpu.HBM)


def near_out(shape, dtype):
    return jax.ShapeDtypeStruct(shape, dtype) if INTERPRET else pltpu.VMEM(shape, dtype)


def copies(piece, count):
    return pl.pallas_call(
        copies_kernel,
        out_shape=near_out((count, *piece.shape), piece.dtype),
        in_specs=[VMEM()],
        out_specs=VMEM(),
        interpret=bool(INTERPRET),
        compiler_params=PARAMS,
        name="copies",
    )(far(piece))


def attend(sizes, lens, table, gathered, pool):
    n_tp, slots, _ = gathered.shape
    return pl.pallas_call(
        attend_kernel,
        out_shape=near_out((n_tp, MSG_ROWS, LANES), BF),
        in_specs=[SMEM(), SMEM(), SMEM(), VMEM(), pl.BlockSpec(memory_space=pltpu.HBM)],
        out_specs=VMEM(),
        scratch_shapes=[
            pltpu.VMEM((slots, table.shape[1], *pool.shape[1:]), BF),
            pltpu.VMEM((n_tp * slots, LANES), F32),
            pltpu.VMEM((slots * n_tp, LANES), F32),
            pltpu.VMEM((n_tp, LANES), F32),
            pltpu.SemaphoreType.DMA((slots, table.shape[1] // CHUNK)),
        ],
        interpret=bool(INTERPRET),
        compiler_params=PARAMS,
        name="attend",
    )(sizes, far(lens), far(table), near(gathered), far(pool))


def combine(sizes, message, own, fresh, pairs):
    n_tp = message.shape[0]
    slots = own.shape[0]
    rows = slots * 2 * len(pairs) // n_tp
    width = -(-pairs[0].shape[0] // 2 // LANES) * LANES
    return pl.pallas_call(
        functools.partial(combine_kernel, tuple(pairs)),
        out_shape=near_out((n_tp, rows, width), BF),
        in_specs=[SMEM()] + [VMEM()] * (3 + len(pairs)),
        out_specs=VMEM(),
        interpret=bool(INTERPRET),
        compiler_params=PARAMS,
        name="combine",
    )(sizes, near(message), near(own), near(fresh), *map(near, pairs.values()))


def total_copies(pieces):
    return pl.pallas_call(
        total_kernel,
        out_shape=near_out(pieces.shape, BF),
        in_specs=[VMEM()],
        out_specs=VMEM(),
        interpret=bool(INTERPRET),
        compiler_params=PARAMS,
        name="total",
    )(near(pieces))


def finish(pieces, slots, width):
    return pl.pallas_call(
        finish_kernel,
        out_shape=jax.ShapeDtypeStruct((1, slots, width), F32),
        in_specs=[VMEM()],
        out_specs=VMEM(),
        interpret=bool(INTERPRET),
        compiler_params=PARAMS,
        name="finish",
    )(near(pieces))


def exchange(pieces, axis):
    return lax.all_to_all(pieces, axis, split_axis=0, concat_axis=0, tiled=True)


def local(batch_sizes, seq_lens, page_table, queries, kv_pool, new_kv, out_weight):
    n_tp = lax.axis_size("tp")
    n_grp = lax.axis_size("grp")
    own = queries[0]
    slots = own.shape[0]

    def from_pair(block, step):
        return lax.ppermute(block, "grp", [(i, i ^ step) for i in range(n_grp)])

    own_block = out_weight.T
    pair = jnp.concatenate([own_block, from_pair(own_block, FIRST_STEP)])
    pairs = {0: pair, **{step: from_pair(pair, step) for step in PAIR_STEPS}}
    fanned = copies(own, n_tp)
    gathered = exchange(fanned, "tp")
    message = attend(batch_sizes, seq_lens[0], page_table[0], gathered, kv_pool[0])
    received = exchange(message, "tp")
    shares = combine(batch_sizes, received, own, new_kv[0], pairs)
    totals = total_copies(exchange(shares, "tp"))
    return finish(exchange(totals, "tp"), slots, n_grp * out_weight.shape[1])


def solution(mesh):
    return jax.shard_map(
        local,
        mesh=mesh,
        in_specs=(
            P("grp"),
            P("grp", None),
            P("grp", None, "tp"),
            P("grp", None, "tp"),
            P("grp", "tp", None, None),
            P("grp", None, None),
            P("tp", "grp"),
        ),
        out_specs=P("grp", None, None),
        check_vma=False,
    )
```

```python
import functools

import jax
import jax.numpy as jnp
from jax import lax
from jax.experimental import pallas as pl
from jax.experimental.pallas import tpu as pltpu
from jax.sharding import PartitionSpec as P


HEADS = 64
KV_HEADS = 8
HD = 64
LANES = 128
NEG_BIG = -1e30
BF = jnp.bfloat16
F32 = jnp.float32
STAT_ROW = 16
MSG_ROWS = 24
INTERPRET = False
FIRST_STEP = 4
PAIR_STEPS = (2, 3, 1)
UNROLL = 2


def axis_index(name):
    return INTERPRET[name] if INTERPRET else lax.axis_index(name)


def lane_iota(rows):
    return lax.broadcasted_iota(jnp.int32, (rows, LANES), 1)


def roll_lanes(x, shift):
    return pltpu.roll(x, shift, 1)


def split_bf(x):
    hi = x.astype(BF)
    lo = (x - hi.astype(F32)).astype(BF)
    return hi, lo


def attend_kernel(
    size_ref, lens_ref, table_ref, q_ref, pool_ref, out_ref, num_scr, stat_scr
):
    slots, pages = table_ref.shape
    n_tp = q_ref.shape[0] // slots
    page_len = pool_ref.shape[1]
    kv_cols = KV_HEADS * HD
    tokens = pages * page_len
    live_count = size_ref[0]
    tp_index = axis_index("tp")
    steps = (live_count + UNROLL - 1) // UNROLL

    def live_length(slot):
        return jnp.where(slot < live_count, lens_ref[slot], 0)

    num_scr[...] = jnp.zeros_like(num_scr)
    low_half = lane_iota(n_tp) < HD
    own_block = (
        lax.broadcasted_iota(jnp.int32, (n_tp, kv_cols), 1) // HD
        == lax.broadcasted_iota(jnp.int32, (n_tp, kv_cols), 0) // (n_tp // KV_HEADS)
    )
    column = lax.broadcasted_iota(jnp.int32, (HEADS, tokens), 1)
    position = (column // page_len) * (page_len * n_tp) + tp_index * page_len + column % page_len
    lane = lane_iota(HEADS)

    def slot_queries(slot):
        x = q_ref[pl.ds(slot, n_tp, stride=slots), :]
        turned = roll_lanes(x, HD)
        even = jnp.where(low_half, x, turned)
        odd = jnp.where(low_half, turned, x)
        wide = [jnp.where(own_block, jnp.concatenate([h] * 4, axis=1), 0.0) for h in (even, odd)]
        return jnp.concatenate(wide, axis=0).astype(BF)

    def slot_scores(slot, ids):
        keys = jnp.concatenate([pool_ref[i, :, 0:kv_cols] for i in ids], axis=0)
        return lax.dot_general(
            slot_queries(slot), keys, (((1,), (1,)), ((), ())), preferred_element_type=F32
        )

    def slot_weights(slot, scores):
        live = position < live_length(slot)
        scores = jnp.where(live, scores, NEG_BIG)
        top = jnp.max(scores, axis=1, keepdims=True)
        top = (top + jnp.abs(top) * 2.0**-7).astype(BF).astype(F32)
        weights = jnp.where(live, jnp.exp(scores - top), 0.0)
        return top, jnp.sum(weights, axis=1, keepdims=True), weights.astype(BF)

    def slot_values(slot, ids, weights):
        values = jnp.concatenate([pool_ref[i, :, kv_cols : 2 * kv_cols] for i in ids], axis=0)
        mixed = jnp.dot(weights, values, preferred_element_type=F32)
        folded = []
        for part in (mixed[:n_tp], mixed[n_tp:]):
            part = jnp.where(own_block, part, 0.0)
            part = sum(part[:, i * LANES : (i + 1) * LANES] for i in range(4))
            folded.append(part + roll_lanes(part, HD))
        num_scr[pl.ds(pl.multiple_of(slot * n_tp, n_tp), n_tp), :] = jnp.where(
            low_half, folded[0], folded[1]
        )

    def some_slots(step, state):
        tops, sums = state
        group = [step * UNROLL + i for i in range(UNROLL)]
        ids = [[table_ref[slot, i] for i in range(pages)] for slot in group]
        scores = [slot_scores(slot, i) for slot, i in zip(group, ids)]
        parts = [slot_weights(slot, s) for slot, s in zip(group, scores)]
        for slot, i, (top, total, weights) in zip(group, ids, parts):
            slot_values(slot, i, weights)
            here = lane == slot
            tops = jnp.where(here, top, tops)
            sums = jnp.where(here, total, sums)
        return tops, sums

    start = (
        jnp.where(lane < slots, NEG_BIG, 0.0).astype(F32),
        jnp.zeros((HEADS, LANES), F32),
    )
    tops, sums = lax.fori_loop(0, steps, some_slots, start)
    hi, lo = split_bf(sums)
    packed = tops + roll_lanes(hi.astype(F32), slots) + roll_lanes(lo.astype(F32), 2 * slots)
    stat_scr[...] = packed[:n_tp] + roll_lanes(packed[n_tp:], HD)
    for t in range(n_tp):
        out_ref[t, 0:slots, :] = num_scr[pl.ds(t, slots, stride=n_tp), :].astype(BF)
        out_ref[t, STAT_ROW:MSG_ROWS, :] = jnp.broadcast_to(
            stat_scr[t : t + 1, :], (MSG_ROWS - STAT_ROW, LANES)
        ).astype(BF)


def merge_kernel(size_ref, msg_ref, q_ref, new_ref, out_ref):
    n_tp = msg_ref.shape[0]
    slots = q_ref.shape[0]
    live_count = size_ref[0]
    tp_index = axis_index("tp")
    ones_block = (
        lax.broadcasted_iota(jnp.int32, (LANES, LANES), 0) // HD
        == lax.broadcasted_iota(jnp.int32, (LANES, LANES), 1) // HD
    ).astype(F32).astype(BF)
    rows8 = MSG_ROWS - STAT_ROW
    stats = [msg_ref[t, STAT_ROW:MSG_ROWS, :].astype(F32) for t in range(n_tp)]
    top = functools.reduce(jnp.maximum, stats)
    scale = [jnp.exp(s - top) for s in stats]
    sums = sum(
        w * (roll_lanes(s, LANES - slots) + roll_lanes(s, LANES - 2 * slots))
        for w, s in zip(scale, stats)
    )
    sub = lax.broadcasted_iota(jnp.int32, (rows8, LANES), 0)
    within = lane_iota(rows8) % HD
    picks = [within == sub + rows8 * i for i in range(slots // rows8)]
    picked = jnp.concatenate(
        [jnp.where(p, v, 0.0) for v in (*scale, top, sums) for p in picks], axis=0
    )
    hi, lo = split_bf(picked)
    spread = jnp.dot(hi, ones_block, preferred_element_type=F32) + jnp.dot(
        lo, ones_block, preferred_element_type=F32
    )
    top_all = spread[n_tp * slots : (n_tp + 1) * slots]
    sum_all = spread[(n_tp + 1) * slots :]
    numerator = sum(
        msg_ref[t, 0:slots, :].astype(F32) * spread[t * slots : (t + 1) * slots]
        for t in range(n_tp)
    )

    kv_head = tp_index // (n_tp // KV_HEADS)
    low_half = lane_iota(slots) < HD

    def own_columns(first):
        at = pl.multiple_of(first + (kv_head // 2) * LANES, LANES)
        block = new_ref[:, pl.ds(at, LANES)].astype(F32)
        turned = roll_lanes(block, HD)
        low = jnp.where(low_half, block, turned)
        high = jnp.where(low_half, turned, block)
        return jnp.where(kv_head % 2 == 0, low, high)

    new_key = own_columns(0)
    new_value = own_columns(KV_HEADS * HD)
    products = q_ref[...].astype(F32) * HD**-0.5 * new_key
    hi, lo = split_bf(products)
    self_score = jnp.dot(hi, ones_block, preferred_element_type=F32) + jnp.dot(
        lo, ones_block, preferred_element_type=F32
    )
    final_top = jnp.maximum(top_all, self_score)
    cached = jnp.exp(top_all - final_top)
    fresh = jnp.exp(self_score - final_top)
    attended = (numerator * cached + new_value * fresh) / (sum_all * cached + fresh)
    slot = lax.broadcasted_iota(jnp.int32, (slots, LANES), 0)
    out_ref[...] = jnp.where(slot < live_count, attended, 0.0).astype(BF)


def project_kernel(offsets, attended_ref, *rest):
    pair_refs, out_ref = rest[:-1], rest[-1]
    grp_index = axis_index("grp")
    attended = attended_ref[...]
    blocks = 2 * len(pair_refs)
    width = pair_refs[0].shape[0] // 2
    parts = out_ref.shape[0] // blocks
    rows = attended.shape[0] // parts
    for offset, pair_ref in zip(offsets, pair_refs):
        for half in range(2):
            share = lax.dot_general(
                attended,
                pair_ref[half * width : (half + 1) * width, :],
                (((1,), (1,)), ((), ())),
                preferred_element_type=F32,
            ).astype(BF)
            block = jnp.bitwise_xor(grp_index, offset ^ (half * FIRST_STEP))
            for i in range(parts):
                out_ref[block * parts + i, :, 0:width] = share[i * rows : (i + 1) * rows]


def rescale_kernel(in_ref, out_ref):
    out_ref[...] = (in_ref[...].astype(F32) * HD**-0.5).reshape(out_ref.shape)


def copies_kernel(size_ref, in_ref, out_ref):
    del size_ref
    out_ref[...] = jnp.broadcast_to(in_ref[...][None], out_ref.shape)


def join_kernel(one_ref, other_ref, out_ref):
    rows = one_ref.shape[0]
    out_ref[0:rows, :] = one_ref[...]
    out_ref[rows : 2 * rows, :] = other_ref[...]


def total_kernel(in_ref, out_ref):
    n_tp = in_ref.shape[0]
    total = sum(in_ref[t].astype(F32) for t in range(n_tp)).astype(BF)
    for t in range(n_tp):
        out_ref[t] = total


def finish_kernel(in_ref, out_ref):
    n_tp, rows, _ = in_ref.shape
    parts = out_ref.shape[1] // rows
    blocks = n_tp // parts
    width = out_ref.shape[2] // blocks
    for b in range(blocks):
        for i in range(parts):
            out_ref[0, i * rows : (i + 1) * rows, b * width : (b + 1) * width] = in_ref[
                b * parts + i, :, 0:width
            ].astype(F32)


SMEM = functools.partial(pl.BlockSpec, memory_space=pltpu.SMEM)
VMEM = functools.partial(pl.BlockSpec, memory_space=pltpu.VMEM)
PARAMS = pltpu.CompilerParams(vmem_limit_bytes=16 << 20)


def near(x):
    return x if INTERPRET else pltpu.with_memory_space_constraint(x, pltpu.VMEM)


def far(x):
    return x if INTERPRET else pltpu.with_memory_space_constraint(x, pltpu.HBM)


def near_out(shape, dtype):
    return jax.ShapeDtypeStruct(shape, dtype) if INTERPRET else pltpu.VMEM(shape, dtype)


def rescale(pieces):
    return pl.pallas_call(
        rescale_kernel,
        out_shape=near_out((pieces.shape[0] * pieces.shape[1], pieces.shape[2]), F32),
        in_specs=[VMEM()],
        out_specs=VMEM(),
        interpret=bool(INTERPRET),
        compiler_params=PARAMS,
        name="rescale",
    )(near(pieces))


def copies(sizes, piece, count):
    return pl.pallas_call(
        copies_kernel,
        out_shape=near_out((count, *piece.shape), piece.dtype),
        in_specs=[SMEM(), VMEM()],
        out_specs=VMEM(),
        interpret=bool(INTERPRET),
        compiler_params=PARAMS,
        cost_estimate=pl.CostEstimate(
            flops=10**11, transcendentals=0, bytes_accessed=piece.size * 2 * (count + 1)
        ),
        name="copies",
    )(sizes, far(piece))


def join(one, other):
    return pl.pallas_call(
        join_kernel,
        out_shape=near_out((2 * one.shape[0], one.shape[1]), one.dtype),
        in_specs=[VMEM()] * 2,
        out_specs=VMEM(),
        interpret=bool(INTERPRET),
        compiler_params=PARAMS,
        name="join",
    )(near(one), near(other))


def attend(sizes, lens, table, scaled, pool):
    slots = table.shape[0]
    n_tp = scaled.shape[0] // slots
    return pl.pallas_call(
        attend_kernel,
        out_shape=near_out((n_tp, MSG_ROWS, LANES), BF),
        in_specs=[SMEM(), SMEM(), SMEM(), VMEM(), VMEM()],
        out_specs=VMEM(),
        scratch_shapes=[
            pltpu.VMEM((slots * n_tp, LANES), F32),
            pltpu.VMEM((n_tp, LANES), F32),
        ],
        interpret=bool(INTERPRET),
        compiler_params=PARAMS,
        name="attend",
    )(sizes, far(lens), far(table), near(scaled), near(pool))


def merge(sizes, message, own, fresh):
    return pl.pallas_call(
        merge_kernel,
        out_shape=near_out(own.shape, BF),
        in_specs=[SMEM()] + [VMEM()] * 3,
        out_specs=VMEM(),
        interpret=bool(INTERPRET),
        compiler_params=PARAMS,
        name="merge",
    )(sizes, near(message), near(own), near(fresh))


def project(attended, pairs, n_tp):
    rows = attended.shape[0] * 2 * len(pairs) // n_tp
    width = -(-pairs[0].shape[0] // 2 // LANES) * LANES
    return pl.pallas_call(
        functools.partial(project_kernel, tuple(pairs)),
        out_shape=near_out((n_tp, rows, width), BF),
        in_specs=[VMEM()] * (1 + len(pairs)),
        out_specs=VMEM(),
        interpret=bool(INTERPRET),
        compiler_params=PARAMS,
        name="project",
    )(near(attended), *map(near, pairs.values()))


def total_copies(pieces):
    return pl.pallas_call(
        total_kernel,
        out_shape=near_out(pieces.shape, BF),
        in_specs=[VMEM()],
        out_specs=VMEM(),
        interpret=bool(INTERPRET),
        compiler_params=PARAMS,
        name="total",
    )(near(pieces))


def finish(pieces, slots, width):
    return pl.pallas_call(
        finish_kernel,
        out_shape=jax.ShapeDtypeStruct((1, slots, width), F32),
        in_specs=[VMEM()],
        out_specs=VMEM(),
        interpret=bool(INTERPRET),
        compiler_params=PARAMS,
        name="finish",
    )(near(pieces))


def exchange(pieces, axis):
    return lax.all_to_all(pieces, axis, split_axis=0, concat_axis=0, tiled=True)


def local(batch_sizes, seq_lens, page_table, queries, kv_pool, new_kv, out_weight):
    n_tp = lax.axis_size("tp")
    n_grp = lax.axis_size("grp")
    own = queries[0]
    slots = own.shape[0]

    def from_pair(block, step):
        return lax.ppermute(block, "grp", [(i, i ^ step) for i in range(n_grp)])

    own_block = out_weight.T
    first = from_pair(own_block, FIRST_STEP)
    fanned = copies(batch_sizes, own, n_tp)
    gathered = exchange(fanned, "tp")
    scaled = rescale(gathered)
    late_block, scaled = lax.optimization_barrier((own_block, scaled))
    pair = join(late_block, first)
    pairs = {0: pair, **{step: from_pair(pair, step) for step in PAIR_STEPS}}
    message = attend(batch_sizes, seq_lens[0], page_table[0], scaled, kv_pool[0])
    received = exchange(message, "tp")
    attended = merge(batch_sizes, received, own, new_kv[0])
    shares = project(attended, pairs, n_tp)
    totals = total_copies(exchange(shares, "tp"))
    return finish(exchange(totals, "tp"), slots, n_grp * out_weight.shape[1])


def solution(mesh):
    return jax.shard_map(
        local,
        mesh=mesh,
        in_specs=(
            P("grp"),
            P("grp", None),
            P("grp", None, "tp"),
            P("grp", None, "tp"),
            P("grp", "tp", None, None),
            P("grp", None, None),
            P("tp", "grp"),
        ),
        out_specs=P("grp", None, None),
        check_vma=False,
    )
```

```python
import functools

import jax
import jax.numpy as jnp
from jax import lax
from jax.experimental import pallas as pl
from jax.experimental.pallas import tpu as pltpu
from jax.sharding import PartitionSpec as P


HEADS = 64
KV_HEADS = 8
HD = 64
LANES = 128
NEG_BIG = -1e30
BF = jnp.bfloat16
F32 = jnp.float32
STAT_ROW = 16
MSG_ROWS = 24
INTERPRET = False
FIRST_STEP = 4
PAIR_STEPS = (2, 3, 1)
UNROLL = 4
CHUNK = 16


def axis_index(name):
    return INTERPRET[name] if INTERPRET else lax.axis_index(name)


def lane_iota(rows):
    return lax.broadcasted_iota(jnp.int32, (rows, LANES), 1)


def roll_lanes(x, shift):
    return pltpu.roll(x, shift, 1)


def split_bf(x):
    hi = x.astype(BF)
    lo = (x - hi.astype(F32)).astype(BF)
    return hi, lo


def attend_kernel(
    size_ref, lens_ref, table_ref, q_ref, pool_ref, out_ref, kv_scr, q_scr, num_scr, stat_scr, sems
):
    n_tp, slots, _ = q_ref.shape
    pages = table_ref.shape[1]
    page_len = pool_ref.shape[1]
    kv_cols = KV_HEADS * HD
    tokens = pages * page_len
    live_count = size_ref[0]
    tp_index = axis_index("tp")
    steps = (live_count + UNROLL - 1) // UNROLL

    def live_length(slot):
        return jnp.where(slot < live_count, lens_ref[slot], 0)

    def is_live(slot, chunk):
        first_page = chunk * CHUNK
        return (first_page * n_tp + tp_index) * page_len < live_length(slot)

    def load_pages(slot):
        for chunk in range(pages // CHUNK):

            @pl.when(is_live(slot, chunk))
            def _():
                for i in range(chunk * CHUNK, (chunk + 1) * CHUNK):
                    pltpu.make_async_copy(
                        pool_ref.at[table_ref[slot, i]],
                        kv_scr.at[slot, i],
                        sems.at[slot, chunk],
                    ).start()

            @pl.when(jnp.logical_not(is_live(slot, chunk)))
            def _():
                kv_scr[slot, chunk * CHUNK : (chunk + 1) * CHUNK, :, kv_cols:] = jnp.zeros(
                    (CHUNK, page_len, kv_cols), BF
                )

    def wait_pages(slot):
        for chunk in range(pages // CHUNK):

            @pl.when(is_live(slot, chunk))
            def _():
                pltpu.make_async_copy(
                    pool_ref.at[pl.ds(0, CHUNK)],
                    kv_scr.at[slot, pl.ds(chunk * CHUNK, CHUNK)],
                    sems.at[slot, chunk],
                ).wait()

    lax.fori_loop(0, steps * UNROLL, lambda slot, _: load_pages(slot), None)
    pad = slots + 1
    for t in range(n_tp):
        q_scr[t * pad : t * pad + slots, :] = q_ref[t].astype(F32) * HD**-0.5
    num_scr[...] = jnp.zeros_like(num_scr)
    low_half = lane_iota(n_tp) < HD
    own_block = (
        lax.broadcasted_iota(jnp.int32, (n_tp, kv_cols), 1) // HD
        == lax.broadcasted_iota(jnp.int32, (n_tp, kv_cols), 0) // (n_tp // KV_HEADS)
    )
    column = lax.broadcasted_iota(jnp.int32, (HEADS, tokens), 1)
    position = (column // page_len) * (page_len * n_tp) + tp_index * page_len + column % page_len
    lane = lane_iota(HEADS)

    def slot_queries(slot):
        x = q_scr[pl.ds(slot, n_tp, stride=pad), :]
        turned = roll_lanes(x, HD)
        even = jnp.where(low_half, x, turned)
        odd = jnp.where(low_half, turned, x)
        wide = [jnp.where(own_block, jnp.concatenate([h] * 4, axis=1), 0.0) for h in (even, odd)]
        return jnp.concatenate(wide, axis=0).astype(BF)

    def slot_scores(slot):
        keys = kv_scr[slot, :, :, 0:kv_cols].reshape(tokens, kv_cols)
        return lax.dot_general(
            slot_queries(slot), keys, (((1,), (1,)), ((), ())), preferred_element_type=F32
        )

    def slot_weights(slot, scores):
        live = position < live_length(slot)
        scores = jnp.where(live, scores, NEG_BIG)
        top = jnp.max(scores, axis=1, keepdims=True)
        top = (top + jnp.abs(top) * 2.0**-7).astype(BF).astype(F32)
        weights = jnp.where(live, jnp.exp(scores - top), 0.0)
        return top, jnp.sum(weights, axis=1, keepdims=True), weights.astype(BF)

    def slot_values(slot, weights):
        values = kv_scr[slot, :, :, kv_cols : 2 * kv_cols].reshape(tokens, kv_cols)
        mixed = jnp.dot(weights, values, preferred_element_type=F32)
        folded = []
        for part in (mixed[:n_tp], mixed[n_tp:]):
            part = jnp.where(own_block, part, 0.0)
            part = sum(part[:, i * LANES : (i + 1) * LANES] for i in range(4))
            folded.append(part + roll_lanes(part, HD))
        num_scr[pl.ds(slot * (n_tp + 1), n_tp), :] = jnp.where(
            low_half, folded[0], folded[1]
        )

    def some_slots(step, state):
        tops, sums = state
        group = [step * UNROLL + i for i in range(UNROLL)]
        for slot in group:
            wait_pages(slot)
        scores = [slot_scores(slot) for slot in group]
        parts = [slot_weights(slot, s) for slot, s in zip(group, scores)]
        for slot, (top, total, weights) in zip(group, parts):
            slot_values(slot, weights)
            here = lane == slot
            tops = jnp.where(here, top, tops)
            sums = jnp.where(here, total, sums)
        return tops, sums

    start = (
        jnp.where(lane < slots, NEG_BIG, 0.0).astype(F32),
        jnp.zeros((HEADS, LANES), F32),
    )
    tops, sums = lax.fori_loop(0, steps, some_slots, start)
    hi, lo = split_bf(sums)
    packed = tops + roll_lanes(hi.astype(F32), slots) + roll_lanes(lo.astype(F32), 2 * slots)
    stat_scr[...] = packed[:n_tp] + roll_lanes(packed[n_tp:], HD)
    for t in range(n_tp):
        out_ref[t, 0:slots, :] = num_scr[pl.ds(t, slots, stride=n_tp + 1), :].astype(BF)
        out_ref[t, STAT_ROW:MSG_ROWS, :] = jnp.broadcast_to(
            stat_scr[t : t + 1, :], (MSG_ROWS - STAT_ROW, LANES)
        ).astype(BF)


def combine_kernel(offsets, size_ref, msg_ref, q_ref, new_ref, *rest):
    pair_refs, out_ref = rest[:-1], rest[-1]
    n_tp = msg_ref.shape[0]
    slots = q_ref.shape[0]
    live_count = size_ref[0]
    tp_index = axis_index("tp")
    grp_index = axis_index("grp")
    blocks = 2 * len(pair_refs)
    width = pair_refs[0].shape[0] // 2
    ones_block = (
        lax.broadcasted_iota(jnp.int32, (LANES, LANES), 0) // HD
        == lax.broadcasted_iota(jnp.int32, (LANES, LANES), 1) // HD
    ).astype(F32).astype(BF)
    rows8 = MSG_ROWS - STAT_ROW
    stats = [msg_ref[t, STAT_ROW:MSG_ROWS, :].astype(F32) for t in range(n_tp)]
    top = functools.reduce(jnp.maximum, stats)
    scale = [jnp.exp(s - top) for s in stats]
    sums = sum(
        w * (roll_lanes(s, LANES - slots) + roll_lanes(s, LANES - 2 * slots))
        for w, s in zip(scale, stats)
    )
    sub = lax.broadcasted_iota(jnp.int32, (rows8, LANES), 0)
    within = lane_iota(rows8) % HD
    picks = [within == sub + rows8 * i for i in range(slots // rows8)]
    picked = jnp.concatenate(
        [jnp.where(p, v, 0.0) for v in (*scale, top, sums) for p in picks], axis=0
    )
    hi, lo = split_bf(picked)
    spread = jnp.dot(hi, ones_block, preferred_element_type=F32) + jnp.dot(
        lo, ones_block, preferred_element_type=F32
    )
    top_all = spread[n_tp * slots : (n_tp + 1) * slots]
    sum_all = spread[(n_tp + 1) * slots :]
    numerator = sum(
        msg_ref[t, 0:slots, :].astype(F32) * spread[t * slots : (t + 1) * slots]
        for t in range(n_tp)
    )

    kv_head = tp_index // (n_tp // KV_HEADS)
    low_half = lane_iota(slots) < HD

    def own_columns(first):
        at = pl.multiple_of(first + (kv_head // 2) * LANES, LANES)
        block = new_ref[:, pl.ds(at, LANES)].astype(F32)
        turned = roll_lanes(block, HD)
        low = jnp.where(low_half, block, turned)
        high = jnp.where(low_half, turned, block)
        return jnp.where(kv_head % 2 == 0, low, high)

    new_key = own_columns(0)
    new_value = own_columns(KV_HEADS * HD)
    products = q_ref[...].astype(F32) * HD**-0.5 * new_key
    hi, lo = split_bf(products)
    self_score = jnp.dot(hi, ones_block, preferred_element_type=F32) + jnp.dot(
        lo, ones_block, preferred_element_type=F32
    )
    final_top = jnp.maximum(top_all, self_score)
    cached = jnp.exp(top_all - final_top)
    fresh = jnp.exp(self_score - final_top)
    attended = (numerator * cached + new_value * fresh) / (sum_all * cached + fresh)
    slot = lax.broadcasted_iota(jnp.int32, (slots, LANES), 0)
    attended = jnp.where(slot < live_count, attended, 0.0).astype(BF)
    parts = n_tp // blocks
    rows = slots // parts
    for offset, pair_ref in zip(offsets, pair_refs):
        for half in range(2):
            share = lax.dot_general(
                attended,
                pair_ref[half * width : (half + 1) * width, :],
                (((1,), (1,)), ((), ())),
                preferred_element_type=F32,
            ).astype(BF)
            block = jnp.bitwise_xor(grp_index, offset ^ (half * FIRST_STEP))
            for i in range(parts):
                out_ref[block * parts + i, :, 0:width] = share[i * rows : (i + 1) * rows]


def copies_kernel(in_ref, out_ref):
    out_ref[...] = jnp.broadcast_to(in_ref[...][None], out_ref.shape)


def join_kernel(one_ref, other_ref, out_ref):
    rows = one_ref.shape[0]
    out_ref[0:rows, :] = one_ref[...]
    out_ref[rows : 2 * rows, :] = other_ref[...]


def total_kernel(in_ref, out_ref):
    n_tp = in_ref.shape[0]
    total = sum(in_ref[t].astype(F32) for t in range(n_tp)).astype(BF)
    for t in range(n_tp):
        out_ref[t] = total


def finish_kernel(in_ref, out_ref):
    n_tp, rows, _ = in_ref.shape
    parts = out_ref.shape[1] // rows
    blocks = n_tp // parts
    width = out_ref.shape[2] // blocks
    for b in range(blocks):
        for i in range(parts):
            out_ref[0, i * rows : (i + 1) * rows, b * width : (b + 1) * width] = in_ref[
                b * parts + i, :, 0:width
            ].astype(F32)


SMEM = functools.partial(pl.BlockSpec, memory_space=pltpu.SMEM)
VMEM = functools.partial(pl.BlockSpec, memory_space=pltpu.VMEM)
PARAMS = pltpu.CompilerParams(vmem_limit_bytes=16 << 20)


def near(x):
    return x if INTERPRET else pltpu.with_memory_space_constraint(x, pltpu.VMEM)


def far(x):
    return x if INTERPRET else pltpu.with_memory_space_constraint(x, pltpu.HBM)


def near_out(shape, dtype):
    return jax.ShapeDtypeStruct(shape, dtype) if INTERPRET else pltpu.VMEM(shape, dtype)


def copies(piece, count):
    return pl.pallas_call(
        copies_kernel,
        out_shape=near_out((count, *piece.shape), piece.dtype),
        in_specs=[VMEM()],
        out_specs=VMEM(),
        interpret=bool(INTERPRET),
        compiler_params=PARAMS,
        cost_estimate=pl.CostEstimate(
            flops=10**11, transcendentals=0, bytes_accessed=piece.size * 2 * (count + 1)
        ),
        name="copies",
    )(far(piece))


def join(one, other):
    return pl.pallas_call(
        join_kernel,
        out_shape=near_out((2 * one.shape[0], one.shape[1]), one.dtype),
        in_specs=[VMEM()] * 2,
        out_specs=VMEM(),
        interpret=bool(INTERPRET),
        compiler_params=PARAMS,
        name="join",
    )(near(one), near(other))


def attend(sizes, lens, table, gathered, pool):
    n_tp, slots, _ = gathered.shape
    return pl.pallas_call(
        attend_kernel,
        out_shape=near_out((n_tp, MSG_ROWS, LANES), BF),
        in_specs=[SMEM(), SMEM(), SMEM(), VMEM(), pl.BlockSpec(memory_space=pltpu.HBM)],
        out_specs=VMEM(),
        scratch_shapes=[
            pltpu.VMEM((slots, table.shape[1], *pool.shape[1:]), BF),
            pltpu.VMEM((n_tp * (slots + 1), LANES), F32),
            pltpu.VMEM((slots * (n_tp + 1), LANES), F32),
            pltpu.VMEM((n_tp, LANES), F32),
            pltpu.SemaphoreType.DMA((slots, table.shape[1] // CHUNK)),
        ],
        interpret=bool(INTERPRET),
        compiler_params=PARAMS,
        name="attend",
    )(sizes, far(lens), far(table), near(gathered), far(pool))


def combine(sizes, message, own, fresh, pairs):
    n_tp = message.shape[0]
    slots = own.shape[0]
    rows = slots * 2 * len(pairs) // n_tp
    width = -(-pairs[0].shape[0] // 2 // LANES) * LANES
    return pl.pallas_call(
        functools.partial(combine_kernel, tuple(pairs)),
        out_shape=near_out((n_tp, rows, width), BF),
        in_specs=[SMEM()] + [VMEM()] * (3 + len(pairs)),
        out_specs=VMEM(),
        interpret=bool(INTERPRET),
        compiler_params=PARAMS,
        name="combine",
    )(sizes, near(message), near(own), near(fresh), *map(near, pairs.values()))


def total_copies(pieces):
    return pl.pallas_call(
        total_kernel,
        out_shape=near_out(pieces.shape, BF),
        in_specs=[VMEM()],
        out_specs=VMEM(),
        interpret=bool(INTERPRET),
        compiler_params=PARAMS,
        name="total",
    )(near(pieces))


def finish(pieces, slots, width):
    return pl.pallas_call(
        finish_kernel,
        out_shape=jax.ShapeDtypeStruct((1, slots, width), F32),
        in_specs=[VMEM()],
        out_specs=VMEM(),
        interpret=bool(INTERPRET),
        compiler_params=PARAMS,
        name="finish",
    )(near(pieces))


def exchange(pieces, axis):
    return lax.all_to_all(pieces, axis, split_axis=0, concat_axis=0, tiled=True)


def local(batch_sizes, seq_lens, page_table, queries, kv_pool, new_kv, out_weight):
    n_tp = lax.axis_size("tp")
    n_grp = lax.axis_size("grp")
    own = queries[0]
    slots = own.shape[0]

    def from_pair(block, step):
        return lax.ppermute(block, "grp", [(i, i ^ step) for i in range(n_grp)])

    own_block = out_weight.T
    pair = join(own_block, from_pair(own_block, FIRST_STEP))
    pairs = {0: pair, **{step: from_pair(pair, step) for step in PAIR_STEPS}}
    fanned = copies(own, n_tp)
    gathered = exchange(fanned, "tp")
    message = attend(batch_sizes, seq_lens[0], page_table[0], gathered, kv_pool[0])
    received = exchange(message, "tp")
    shares = combine(batch_sizes, received, own, new_kv[0], pairs)
    totals = total_copies(exchange(shares, "tp"))
    return finish(exchange(totals, "tp"), slots, n_grp * out_weight.shape[1])


def solution(mesh):
    return jax.shard_map(
        local,
        mesh=mesh,
        in_specs=(
            P("grp"),
            P("grp", None),
            P("grp", None, "tp"),
            P("grp", None, "tp"),
            P("grp", "tp", None, None),
            P("grp", None, None),
            P("tp", "grp"),
        ),
        out_specs=P("grp", None, None),
        check_vma=False,
    )
```

```python
import functools

import jax
import jax.numpy as jnp
from jax import lax
from jax.experimental import pallas as pl
from jax.experimental.pallas import tpu as pltpu
from jax.sharding import PartitionSpec as P


HEADS = 64
KV_HEADS = 8
HD = 64
LANES = 128
NEG_BIG = -1e30
BF = jnp.bfloat16
F32 = jnp.float32
STAT_ROW = 16
MSG_ROWS = 24
INTERPRET = False
FIRST_STEP = 4
PAIR_STEPS = (2, 3, 1)
UNROLL = 4
CHUNK = 16


def axis_index(name):
    return INTERPRET[name] if INTERPRET else lax.axis_index(name)


def lane_iota(rows):
    return lax.broadcasted_iota(jnp.int32, (rows, LANES), 1)


def roll_lanes(x, shift):
    return pltpu.roll(x, shift, 1)


def split_bf(x):
    hi = x.astype(BF)
    lo = (x - hi.astype(F32)).astype(BF)
    return hi, lo


def attend_kernel(
    size_ref, lens_ref, table_ref, q_ref, pool_ref, out_ref, kv_scr, q_scr, num_scr, stat_scr, sems
):
    n_tp, slots, _ = q_ref.shape
    pages = table_ref.shape[1]
    page_len = pool_ref.shape[1]
    kv_cols = KV_HEADS * HD
    tokens = pages * page_len
    live_count = size_ref[0]
    tp_index = axis_index("tp")
    steps = (live_count + UNROLL - 1) // UNROLL

    def live_length(slot):
        return jnp.where(slot < live_count, lens_ref[slot], 0)

    def is_live(slot, chunk):
        first_page = chunk * CHUNK
        return (first_page * n_tp + tp_index) * page_len < live_length(slot)

    def load_pages(slot):
        for chunk in range(pages // CHUNK):

            @pl.when(is_live(slot, chunk))
            def _():
                for i in range(chunk * CHUNK, (chunk + 1) * CHUNK):
                    pltpu.make_async_copy(
                        pool_ref.at[table_ref[slot, i]],
                        kv_scr.at[slot, i],
                        sems.at[slot, chunk],
                    ).start()

            @pl.when(jnp.logical_not(is_live(slot, chunk)))
            def _():
                kv_scr[slot, chunk * CHUNK : (chunk + 1) * CHUNK, :, kv_cols:] = jnp.zeros(
                    (CHUNK, page_len, kv_cols), BF
                )

    def wait_pages(slot):
        for chunk in range(pages // CHUNK):

            @pl.when(is_live(slot, chunk))
            def _():
                pltpu.make_async_copy(
                    pool_ref.at[pl.ds(0, CHUNK)],
                    kv_scr.at[slot, pl.ds(chunk * CHUNK, CHUNK)],
                    sems.at[slot, chunk],
                ).wait()

    lax.fori_loop(0, steps * UNROLL, lambda slot, _: load_pages(slot), None)
    pad = slots + 1
    for t in range(n_tp):
        q_scr[t * pad : t * pad + slots, :] = q_ref[t].astype(F32) * HD**-0.5
    num_scr[...] = jnp.zeros_like(num_scr)
    low_half = lane_iota(n_tp) < HD
    own_block = (
        lax.broadcasted_iota(jnp.int32, (n_tp, kv_cols), 1) // HD
        == lax.broadcasted_iota(jnp.int32, (n_tp, kv_cols), 0) // (n_tp // KV_HEADS)
    )
    column = lax.broadcasted_iota(jnp.int32, (HEADS, tokens), 1)
    position = (column // page_len) * (page_len * n_tp) + tp_index * page_len + column % page_len
    lane = lane_iota(HEADS)

    def slot_queries(slot):
        x = q_scr[pl.ds(slot, n_tp, stride=pad), :]
        turned = roll_lanes(x, HD)
        even = jnp.where(low_half, x, turned)
        odd = jnp.where(low_half, turned, x)
        wide = [jnp.where(own_block, jnp.concatenate([h] * 4, axis=1), 0.0) for h in (even, odd)]
        return jnp.concatenate(wide, axis=0).astype(BF)

    def slot_scores(slot):
        keys = kv_scr[slot, :, :, 0:kv_cols].reshape(tokens, kv_cols)
        return lax.dot_general(
            slot_queries(slot), keys, (((1,), (1,)), ((), ())), preferred_element_type=F32
        )

    def slot_weights(slot, scores):
        live = position < live_length(slot)
        scores = jnp.where(live, scores, NEG_BIG)
        top = jnp.max(scores, axis=1, keepdims=True)
        top = (top + jnp.abs(top) * 2.0**-7).astype(BF).astype(F32)
        weights = jnp.where(live, jnp.exp(scores - top), 0.0)
        return top, jnp.sum(weights, axis=1, keepdims=True), weights.astype(BF)

    def slot_values(slot, weights):
        values = kv_scr[slot, :, :, kv_cols : 2 * kv_cols].reshape(tokens, kv_cols)
        mixed = jnp.dot(weights, values, preferred_element_type=F32)
        folded = []
        for part in (mixed[:n_tp], mixed[n_tp:]):
            part = jnp.where(own_block, part, 0.0)
            part = sum(part[:, i * LANES : (i + 1) * LANES] for i in range(4))
            folded.append(part + roll_lanes(part, HD))
        num_scr[pl.ds(slot * (n_tp + 1), n_tp), :] = jnp.where(
            low_half, folded[0], folded[1]
        )

    def some_slots(step, state):
        tops, sums = state
        group = [step * UNROLL + i for i in range(UNROLL)]
        for slot in group:
            wait_pages(slot)
        scores = [slot_scores(slot) for slot in group]
        parts = [slot_weights(slot, s) for slot, s in zip(group, scores)]
        for slot, (top, total, weights) in zip(group, parts):
            slot_values(slot, weights)
            here = lane == slot
            tops = jnp.where(here, top, tops)
            sums = jnp.where(here, total, sums)
        return tops, sums

    start = (
        jnp.where(lane < slots, NEG_BIG, 0.0).astype(F32),
        jnp.zeros((HEADS, LANES), F32),
    )
    tops, sums = lax.fori_loop(0, steps, some_slots, start)
    hi, lo = split_bf(sums)
    packed = tops + roll_lanes(hi.astype(F32), slots) + roll_lanes(lo.astype(F32), 2 * slots)
    stat_scr[...] = packed[:n_tp] + roll_lanes(packed[n_tp:], HD)
    for t in range(n_tp):
        out_ref[t, 0:slots, :] = num_scr[pl.ds(t, slots, stride=n_tp + 1), :].astype(BF)
        out_ref[t, STAT_ROW:MSG_ROWS, :] = jnp.broadcast_to(
            stat_scr[t : t + 1, :], (MSG_ROWS - STAT_ROW, LANES)
        ).astype(BF)


def merge_kernel(size_ref, msg_ref, q_ref, new_ref, out_ref):
    n_tp = msg_ref.shape[0]
    slots = q_ref.shape[0]
    live_count = size_ref[0]
    tp_index = axis_index("tp")
    ones_block = (
        lax.broadcasted_iota(jnp.int32, (LANES, LANES), 0) // HD
        == lax.broadcasted_iota(jnp.int32, (LANES, LANES), 1) // HD
    ).astype(F32).astype(BF)
    rows8 = MSG_ROWS - STAT_ROW
    stats = [msg_ref[t, STAT_ROW:MSG_ROWS, :].astype(F32) for t in range(n_tp)]
    top = functools.reduce(jnp.maximum, stats)
    scale = [jnp.exp(s - top) for s in stats]
    sums = sum(
        w * (roll_lanes(s, LANES - slots) + roll_lanes(s, LANES - 2 * slots))
        for w, s in zip(scale, stats)
    )
    sub = lax.broadcasted_iota(jnp.int32, (rows8, LANES), 0)
    within = lane_iota(rows8) % HD
    picks = [within == sub + rows8 * i for i in range(slots // rows8)]
    picked = jnp.concatenate(
        [jnp.where(p, v, 0.0) for v in (*scale, top, sums) for p in picks], axis=0
    )
    hi, lo = split_bf(picked)
    spread = jnp.dot(hi, ones_block, preferred_element_type=F32) + jnp.dot(
        lo, ones_block, preferred_element_type=F32
    )
    top_all = spread[n_tp * slots : (n_tp + 1) * slots]
    sum_all = spread[(n_tp + 1) * slots :]
    numerator = sum(
        msg_ref[t, 0:slots, :].astype(F32) * spread[t * slots : (t + 1) * slots]
        for t in range(n_tp)
    )

    kv_head = tp_index // (n_tp // KV_HEADS)
    low_half = lane_iota(slots) < HD

    def own_columns(first):
        at = pl.multiple_of(first + (kv_head // 2) * LANES, LANES)
        block = new_ref[:, pl.ds(at, LANES)].astype(F32)
        turned = roll_lanes(block, HD)
        low = jnp.where(low_half, block, turned)
        high = jnp.where(low_half, turned, block)
        return jnp.where(kv_head % 2 == 0, low, high)

    new_key = own_columns(0)
    new_value = own_columns(KV_HEADS * HD)
    products = q_ref[...].astype(F32) * HD**-0.5 * new_key
    hi, lo = split_bf(products)
    self_score = jnp.dot(hi, ones_block, preferred_element_type=F32) + jnp.dot(
        lo, ones_block, preferred_element_type=F32
    )
    final_top = jnp.maximum(top_all, self_score)
    cached = jnp.exp(top_all - final_top)
    fresh = jnp.exp(self_score - final_top)
    attended = (numerator * cached + new_value * fresh) / (sum_all * cached + fresh)
    slot = lax.broadcasted_iota(jnp.int32, (slots, LANES), 0)
    out_ref[...] = jnp.where(slot < live_count, attended, 0.0).astype(BF)


def project_kernel(offsets, attended_ref, *rest):
    pair_refs, out_ref = rest[:-1], rest[-1]
    grp_index = axis_index("grp")
    attended = attended_ref[...]
    blocks = 2 * len(pair_refs)
    width = pair_refs[0].shape[0] // 2
    parts = out_ref.shape[0] // blocks
    rows = attended.shape[0] // parts
    for offset, pair_ref in zip(offsets, pair_refs):
        for half in range(2):
            share = lax.dot_general(
                attended,
                pair_ref[half * width : (half + 1) * width, :],
                (((1,), (1,)), ((), ())),
                preferred_element_type=F32,
            ).astype(BF)
            block = jnp.bitwise_xor(grp_index, offset ^ (half * FIRST_STEP))
            for i in range(parts):
                out_ref[block * parts + i, :, 0:width] = share[i * rows : (i + 1) * rows]


def copies_kernel(in_ref, out_ref):
    out_ref[...] = jnp.broadcast_to(in_ref[...][None], out_ref.shape)


def join_kernel(one_ref, other_ref, out_ref):
    rows = one_ref.shape[0]
    out_ref[0:rows, :] = one_ref[...]
    out_ref[rows : 2 * rows, :] = other_ref[...]


def total_kernel(in_ref, out_ref):
    n_tp = in_ref.shape[0]
    total = sum(in_ref[t].astype(F32) for t in range(n_tp)).astype(BF)
    for t in range(n_tp):
        out_ref[t] = total


def finish_kernel(in_ref, out_ref):
    n_tp, rows, _ = in_ref.shape
    parts = out_ref.shape[1] // rows
    blocks = n_tp // parts
    width = out_ref.shape[2] // blocks
    for b in range(blocks):
        for i in range(parts):
            out_ref[0, i * rows : (i + 1) * rows, b * width : (b + 1) * width] = in_ref[
                b * parts + i, :, 0:width
            ].astype(F32)


SMEM = functools.partial(pl.BlockSpec, memory_space=pltpu.SMEM)
VMEM = functools.partial(pl.BlockSpec, memory_space=pltpu.VMEM)
PARAMS = pltpu.CompilerParams(vmem_limit_bytes=16 << 20)


def near(x):
    return x if INTERPRET else pltpu.with_memory_space_constraint(x, pltpu.VMEM)


def far(x):
    return x if INTERPRET else pltpu.with_memory_space_constraint(x, pltpu.HBM)


def near_out(shape, dtype):
    return jax.ShapeDtypeStruct(shape, dtype) if INTERPRET else pltpu.VMEM(shape, dtype)


def copies(piece, count):
    return pl.pallas_call(
        copies_kernel,
        out_shape=near_out((count, *piece.shape), piece.dtype),
        in_specs=[VMEM()],
        out_specs=VMEM(),
        interpret=bool(INTERPRET),
        compiler_params=PARAMS,
        cost_estimate=pl.CostEstimate(
            flops=10**11, transcendentals=0, bytes_accessed=piece.size * 2 * (count + 1)
        ),
        name="copies",
    )(far(piece))


def join(one, other):
    return pl.pallas_call(
        join_kernel,
        out_shape=near_out((2 * one.shape[0], one.shape[1]), one.dtype),
        in_specs=[VMEM()] * 2,
        out_specs=VMEM(),
        interpret=bool(INTERPRET),
        compiler_params=PARAMS,
        name="join",
    )(near(one), near(other))


def attend(sizes, lens, table, gathered, pool):
    n_tp, slots, _ = gathered.shape
    return pl.pallas_call(
        attend_kernel,
        out_shape=near_out((n_tp, MSG_ROWS, LANES), BF),
        in_specs=[SMEM(), SMEM(), SMEM(), VMEM(), pl.BlockSpec(memory_space=pltpu.HBM)],
        out_specs=VMEM(),
        scratch_shapes=[
            pltpu.VMEM((slots, table.shape[1], *pool.shape[1:]), BF),
            pltpu.VMEM((n_tp * (slots + 1), LANES), F32),
            pltpu.VMEM((slots * (n_tp + 1), LANES), F32),
            pltpu.VMEM((n_tp, LANES), F32),
            pltpu.SemaphoreType.DMA((slots, table.shape[1] // CHUNK)),
        ],
        interpret=bool(INTERPRET),
        compiler_params=PARAMS,
        name="attend",
    )(sizes, far(lens), far(table), near(gathered), far(pool))


def merge(sizes, message, own, fresh):
    return pl.pallas_call(
        merge_kernel,
        out_shape=near_out(own.shape, BF),
        in_specs=[SMEM()] + [VMEM()] * 3,
        out_specs=VMEM(),
        interpret=bool(INTERPRET),
        compiler_params=PARAMS,
        name="merge",
    )(sizes, near(message), near(own), near(fresh))


def project(attended, pairs, n_tp):
    rows = attended.shape[0] * 2 * len(pairs) // n_tp
    width = -(-pairs[0].shape[0] // 2 // LANES) * LANES
    return pl.pallas_call(
        functools.partial(project_kernel, tuple(pairs)),
        out_shape=near_out((n_tp, rows, width), BF),
        in_specs=[VMEM()] * (1 + len(pairs)),
        out_specs=VMEM(),
        interpret=bool(INTERPRET),
        compiler_params=PARAMS,
        name="project",
    )(near(attended), *map(near, pairs.values()))


def total_copies(pieces):
    return pl.pallas_call(
        total_kernel,
        out_shape=near_out(pieces.shape, BF),
        in_specs=[VMEM()],
        out_specs=VMEM(),
        interpret=bool(INTERPRET),
        compiler_params=PARAMS,
        name="total",
    )(near(pieces))


def finish(pieces, slots, width):
    return pl.pallas_call(
        finish_kernel,
        out_shape=jax.ShapeDtypeStruct((1, slots, width), F32),
        in_specs=[VMEM()],
        out_specs=VMEM(),
        interpret=bool(INTERPRET),
        compiler_params=PARAMS,
        name="finish",
    )(near(pieces))


def exchange(pieces, axis):
    return lax.all_to_all(pieces, axis, split_axis=0, concat_axis=0, tiled=True)


def local(batch_sizes, seq_lens, page_table, queries, kv_pool, new_kv, out_weight):
    n_tp = lax.axis_size("tp")
    n_grp = lax.axis_size("grp")
    own = queries[0]
    slots = own.shape[0]

    def from_pair(block, step):
        return lax.ppermute(block, "grp", [(i, i ^ step) for i in range(n_grp)])

    own_block = out_weight.T
    pair = join(own_block, from_pair(own_block, FIRST_STEP))
    pairs = {0: pair, **{step: from_pair(pair, step) for step in PAIR_STEPS}}
    fanned = copies(own, n_tp)
    gathered = exchange(fanned, "tp")
    message = attend(batch_sizes, seq_lens[0], page_table[0], gathered, kv_pool[0])
    received = exchange(message, "tp")
    attended = merge(batch_sizes, received, own, new_kv[0])
    shares = project(attended, pairs, n_tp)
    totals = total_copies(exchange(shares, "tp"))
    return finish(exchange(totals, "tp"), slots, n_grp * out_weight.shape[1])


def solution(mesh):
    return jax.shard_map(
        local,
        mesh=mesh,
        in_specs=(
            P("grp"),
            P("grp", None),
            P("grp", None, "tp"),
            P("grp", None, "tp"),
            P("grp", "tp", None, None),
            P("grp", None, None),
            P("tp", "grp"),
        ),
        out_specs=P("grp", None, None),
        check_vma=False,
    )
```

```python
import functools

import jax
import jax.numpy as jnp
from jax import lax
from jax.experimental import pallas as pl
from jax.experimental.pallas import tpu as pltpu
from jax.sharding import PartitionSpec as P


HEADS = 64
KV_HEADS = 8
HD = 64
LANES = 128
NEG_BIG = -1e30
BF = jnp.bfloat16
F32 = jnp.float32
ROWS = 2
INTERPRET = False
FIRST_STEP = 4
PAIR_STEPS = (2, 3, 1)
UNROLL = 4
CHUNK = 16


def axis_index(name):
    return INTERPRET[name] if INTERPRET else lax.axis_index(name)


def lane_iota(rows):
    return lax.broadcasted_iota(jnp.int32, (rows, LANES), 1)


def roll_lanes(x, shift):
    return pltpu.roll(x, shift, 1)


def split_bf(x):
    hi = x.astype(BF)
    lo = (x - hi.astype(F32)).astype(BF)
    return hi, lo


def attend_kernel(
    size_ref, lens_ref, table_ref, q_ref, pool_ref, out_ref, kv_scr, q_scr, num_scr, stat_scr, sems
):
    n_tp, slots, _ = q_ref.shape
    pages = table_ref.shape[1]
    page_len = pool_ref.shape[1]
    kv_cols = KV_HEADS * HD
    tokens = pages * page_len
    live_count = size_ref[0]
    tp_index = axis_index("tp")
    steps = (live_count + UNROLL - 1) // UNROLL

    def live_length(slot):
        return jnp.where(slot < live_count, lens_ref[slot], 0)

    def is_live(slot, chunk):
        first_page = chunk * CHUNK
        return (first_page * n_tp + tp_index) * page_len < live_length(slot)

    def load_pages(slot):
        for chunk in range(pages // CHUNK):

            @pl.when(is_live(slot, chunk))
            def _():
                for i in range(chunk * CHUNK, (chunk + 1) * CHUNK):
                    pltpu.make_async_copy(
                        pool_ref.at[table_ref[slot, i]],
                        kv_scr.at[slot, i],
                        sems.at[slot, chunk],
                    ).start()

            @pl.when(jnp.logical_not(is_live(slot, chunk)))
            def _():
                kv_scr[slot, chunk * CHUNK : (chunk + 1) * CHUNK, :, kv_cols:] = jnp.zeros(
                    (CHUNK, page_len, kv_cols), BF
                )

    def wait_pages(slot):
        for chunk in range(pages // CHUNK):

            @pl.when(is_live(slot, chunk))
            def _():
                pltpu.make_async_copy(
                    pool_ref.at[pl.ds(0, CHUNK)],
                    kv_scr.at[slot, pl.ds(chunk * CHUNK, CHUNK)],
                    sems.at[slot, chunk],
                ).wait()

    lax.fori_loop(0, steps * UNROLL, lambda slot, _: load_pages(slot), None)
    pad = slots + 1
    for t in range(n_tp):
        q_scr[t * pad : t * pad + slots, :] = q_ref[t].astype(F32) * HD**-0.5
    num_scr[...] = jnp.zeros_like(num_scr)
    low_half = lane_iota(n_tp) < HD
    own_block = (
        lax.broadcasted_iota(jnp.int32, (n_tp, kv_cols), 1) // HD
        == lax.broadcasted_iota(jnp.int32, (n_tp, kv_cols), 0) // (n_tp // KV_HEADS)
    )
    column = lax.broadcasted_iota(jnp.int32, (HEADS, tokens), 1)
    position = (column // page_len) * (page_len * n_tp) + tp_index * page_len + column % page_len
    lane = lane_iota(HEADS)

    def slot_queries(slot):
        x = q_scr[pl.ds(slot, n_tp, stride=pad), :]
        turned = roll_lanes(x, HD)
        even = jnp.where(low_half, x, turned)
        odd = jnp.where(low_half, turned, x)
        wide = [jnp.where(own_block, jnp.concatenate([h] * 4, axis=1), 0.0) for h in (even, odd)]
        return jnp.concatenate(wide, axis=0).astype(BF)

    def slot_scores(slot):
        keys = kv_scr[slot, :, :, 0:kv_cols].reshape(tokens, kv_cols)
        return lax.dot_general(
            slot_queries(slot), keys, (((1,), (1,)), ((), ())), preferred_element_type=F32
        )

    def slot_weights(slot, scores):
        live = position < live_length(slot)
        scores = jnp.where(live, scores, NEG_BIG)
        top = jnp.max(scores, axis=1, keepdims=True)
        top = (top + jnp.abs(top) * 2.0**-7).astype(BF).astype(F32)
        weights = jnp.where(live, jnp.exp(scores - top), 0.0)
        return top, jnp.sum(weights, axis=1, keepdims=True), weights.astype(BF)

    def slot_values(slot, weights):
        values = kv_scr[slot, :, :, kv_cols : 2 * kv_cols].reshape(tokens, kv_cols)
        mixed = jnp.dot(weights, values, preferred_element_type=F32)
        folded = []
        for part in (mixed[:n_tp], mixed[n_tp:]):
            part = jnp.where(own_block, part, 0.0)
            part = sum(part[:, i * LANES : (i + 1) * LANES] for i in range(4))
            folded.append(part + roll_lanes(part, HD))
        num_scr[pl.ds(slot * (n_tp + 1), n_tp), :] = jnp.where(
            low_half, folded[0], folded[1]
        )

    def some_slots(step, state):
        tops, sums = state
        group = [step * UNROLL + i for i in range(UNROLL)]
        for slot in group:
            wait_pages(slot)
        scores = [slot_scores(slot) for slot in group]
        parts = [slot_weights(slot, s) for slot, s in zip(group, scores)]
        for slot, (top, total, weights) in zip(group, parts):
            slot_values(slot, weights)
            here = lane == slot
            tops = jnp.where(here, top, tops)
            sums = jnp.where(here, total, sums)
        return tops, sums

    start = (
        jnp.where(lane < slots, NEG_BIG, 0.0).astype(F32),
        jnp.zeros((HEADS, LANES), F32),
    )
    tops, sums = lax.fori_loop(0, steps, some_slots, start)
    hi, lo = split_bf(sums)
    packed = tops + roll_lanes(hi.astype(F32), slots) + roll_lanes(lo.astype(F32), 2 * slots)
    stat_scr[...] = packed[:n_tp] + roll_lanes(packed[n_tp:], HD)
    for t in range(n_tp):
        for i in range(slots // ROWS):
            pick = pl.ds(i * ROWS * (n_tp + 1) + t, ROWS, stride=n_tp + 1)
            out_ref[t, :, i * LANES : (i + 1) * LANES] = num_scr[pick, :].astype(BF)
        out_ref[t, :, slots // ROWS * LANES :] = jnp.broadcast_to(
            stat_scr[t : t + 1, :], (ROWS, LANES)
        ).astype(BF)


def merge_kernel(size_ref, msg_ref, q_ref, new_ref, out_ref, msg_scr):
    n_tp = msg_ref.shape[0]
    slots = q_ref.shape[0]
    live_count = size_ref[0]
    tp_index = axis_index("tp")
    ones_block = (
        lax.broadcasted_iota(jnp.int32, (LANES, LANES), 0) // HD
        == lax.broadcasted_iota(jnp.int32, (LANES, LANES), 1) // HD
    ).astype(F32).astype(BF)
    rows8 = 8
    stats = []
    for t in range(n_tp):
        for i in range(slots // ROWS):
            msg_scr[t * slots + i * ROWS : t * slots + (i + 1) * ROWS, :] = msg_ref[
                t, :, i * LANES : (i + 1) * LANES
            ].astype(F32)
        stat = msg_ref[t, :, slots // ROWS * LANES :].astype(F32)
        stats.append(jnp.broadcast_to(stat[0:1], (rows8, LANES)))
    top = functools.reduce(jnp.maximum, stats)
    scale = [jnp.exp(s - top) for s in stats]
    sums = sum(
        w * (roll_lanes(s, LANES - slots) + roll_lanes(s, LANES - 2 * slots))
        for w, s in zip(scale, stats)
    )
    sub = lax.broadcasted_iota(jnp.int32, (rows8, LANES), 0)
    within = lane_iota(rows8) % HD
    picks = [within == sub + rows8 * i for i in range(slots // rows8)]
    picked = jnp.concatenate(
        [jnp.where(p, v, 0.0) for v in (*scale, top, sums) for p in picks], axis=0
    )
    hi, lo = split_bf(picked)
    spread = jnp.dot(hi, ones_block, preferred_element_type=F32) + jnp.dot(
        lo, ones_block, preferred_element_type=F32
    )
    top_all = spread[n_tp * slots : (n_tp + 1) * slots]
    sum_all = spread[(n_tp + 1) * slots :]
    numerator = sum(
        msg_scr[t * slots : (t + 1) * slots, :] * spread[t * slots : (t + 1) * slots]
        for t in range(n_tp)
    )

    kv_head = tp_index // (n_tp // KV_HEADS)
    low_half = lane_iota(slots) < HD

    def own_columns(first):
        at = pl.multiple_of(first + (kv_head // 2) * LANES, LANES)
        block = new_ref[:, pl.ds(at, LANES)].astype(F32)
        turned = roll_lanes(block, HD)
        low = jnp.where(low_half, block, turned)
        high = jnp.where(low_half, turned, block)
        return jnp.where(kv_head % 2 == 0, low, high)

    new_key = own_columns(0)
    new_value = own_columns(KV_HEADS * HD)
    products = q_ref[...].astype(F32) * HD**-0.5 * new_key
    hi, lo = split_bf(products)
    self_score = jnp.dot(hi, ones_block, preferred_element_type=F32) + jnp.dot(
        lo, ones_block, preferred_element_type=F32
    )
    final_top = jnp.maximum(top_all, self_score)
    cached = jnp.exp(top_all - final_top)
    fresh = jnp.exp(self_score - final_top)
    attended = (numerator * cached + new_value * fresh) / (sum_all * cached + fresh)
    slot = lax.broadcasted_iota(jnp.int32, (slots, LANES), 0)
    out_ref[...] = jnp.where(slot < live_count, attended, 0.0).astype(BF)


def project_kernel(offsets, attended_ref, *rest):
    pair_refs, out_ref = rest[:-1], rest[-1]
    grp_index = axis_index("grp")
    attended = attended_ref[...]
    blocks = 2 * len(pair_refs)
    width = pair_refs[0].shape[0] // 2
    parts = out_ref.shape[0] // blocks
    rows = attended.shape[0] // parts
    for offset, pair_ref in zip(offsets, pair_refs):
        for half in range(2):
            share = lax.dot_general(
                attended,
                pair_ref[half * width : (half + 1) * width, :],
                (((1,), (1,)), ((), ())),
                preferred_element_type=F32,
            ).astype(BF)
            block = jnp.bitwise_xor(grp_index, offset ^ (half * FIRST_STEP))
            for i in range(parts):
                out_ref[block * parts + i, :, 0:width] = share[i * rows : (i + 1) * rows]


def copies_kernel(in_ref, out_ref):
    out_ref[...] = jnp.broadcast_to(in_ref[...][None], out_ref.shape)


def join_kernel(one_ref, other_ref, out_ref):
    rows = one_ref.shape[0]
    out_ref[0:rows, :] = one_ref[...]
    out_ref[rows : 2 * rows, :] = other_ref[...]


def total_kernel(in_ref, out_ref):
    n_tp = in_ref.shape[0]
    total = sum(in_ref[t].astype(F32) for t in range(n_tp)).astype(BF)
    for t in range(n_tp):
        out_ref[t] = total


def finish_kernel(in_ref, out_ref):
    n_tp, rows, _ = in_ref.shape
    parts = out_ref.shape[1] // rows
    blocks = n_tp // parts
    width = out_ref.shape[2] // blocks
    for b in range(blocks):
        for i in range(parts):
            out_ref[0, i * rows : (i + 1) * rows, b * width : (b + 1) * width] = in_ref[
                b * parts + i, :, 0:width
            ].astype(F32)


SMEM = functools.partial(pl.BlockSpec, memory_space=pltpu.SMEM)
VMEM = functools.partial(pl.BlockSpec, memory_space=pltpu.VMEM)
PARAMS = pltpu.CompilerParams(vmem_limit_bytes=16 << 20)


def near(x):
    return x if INTERPRET else pltpu.with_memory_space_constraint(x, pltpu.VMEM)


def far(x):
    return x if INTERPRET else pltpu.with_memory_space_constraint(x, pltpu.HBM)


def near_out(shape, dtype):
    return jax.ShapeDtypeStruct(shape, dtype) if INTERPRET else pltpu.VMEM(shape, dtype)


def copies(piece, count):
    return pl.pallas_call(
        copies_kernel,
        out_shape=near_out((count, *piece.shape), piece.dtype),
        in_specs=[VMEM()],
        out_specs=VMEM(),
        interpret=bool(INTERPRET),
        compiler_params=PARAMS,
        cost_estimate=pl.CostEstimate(
            flops=10**11, transcendentals=0, bytes_accessed=piece.size * 2 * (count + 1)
        ),
        name="copies",
    )(far(piece))


def join(one, other):
    return pl.pallas_call(
        join_kernel,
        out_shape=near_out((2 * one.shape[0], one.shape[1]), one.dtype),
        in_specs=[VMEM()] * 2,
        out_specs=VMEM(),
        interpret=bool(INTERPRET),
        compiler_params=PARAMS,
        name="join",
    )(near(one), near(other))


def attend(sizes, lens, table, gathered, pool):
    n_tp, slots, _ = gathered.shape
    return pl.pallas_call(
        attend_kernel,
        out_shape=near_out((n_tp, ROWS, (slots // ROWS + 1) * LANES), BF),
        in_specs=[SMEM(), SMEM(), SMEM(), VMEM(), pl.BlockSpec(memory_space=pltpu.HBM)],
        out_specs=VMEM(),
        scratch_shapes=[
            pltpu.VMEM((slots, table.shape[1], *pool.shape[1:]), BF),
            pltpu.VMEM((n_tp * (slots + 1), LANES), F32),
            pltpu.VMEM((slots * (n_tp + 1), LANES), F32),
            pltpu.VMEM((n_tp, LANES), F32),
            pltpu.SemaphoreType.DMA((slots, table.shape[1] // CHUNK)),
        ],
        interpret=bool(INTERPRET),
        compiler_params=PARAMS,
        name="attend",
    )(sizes, near(lens), near(table), near(gathered), far(pool))


def merge(sizes, message, own, fresh):
    return pl.pallas_call(
        merge_kernel,
        out_shape=near_out(own.shape, BF),
        in_specs=[SMEM()] + [VMEM()] * 3,
        out_specs=VMEM(),
        scratch_shapes=[pltpu.VMEM((message.shape[0] * own.shape[0] + 8, LANES), F32)],
        interpret=bool(INTERPRET),
        compiler_params=PARAMS,
        name="merge",
    )(sizes, near(message), near(own), near(fresh))


def project(attended, pairs, n_tp):
    rows = attended.shape[0] * 2 * len(pairs) // n_tp
    width = -(-pairs[0].shape[0] // 2 // LANES) * LANES
    return pl.pallas_call(
        functools.partial(project_kernel, tuple(pairs)),
        out_shape=near_out((n_tp, rows, width), BF),
        in_specs=[VMEM()] * (1 + len(pairs)),
        out_specs=VMEM(),
        interpret=bool(INTERPRET),
        compiler_params=PARAMS,
        name="project",
    )(near(attended), *map(near, pairs.values()))


def total_copies(pieces):
    return pl.pallas_call(
        total_kernel,
        out_shape=near_out(pieces.shape, BF),
        in_specs=[VMEM()],
        out_specs=VMEM(),
        interpret=bool(INTERPRET),
        compiler_params=PARAMS,
        name="total",
    )(near(pieces))


def finish(pieces, slots, width):
    return pl.pallas_call(
        finish_kernel,
        out_shape=jax.ShapeDtypeStruct((1, slots, width), F32),
        in_specs=[VMEM()],
        out_specs=VMEM(),
        interpret=bool(INTERPRET),
        compiler_params=PARAMS,
        name="finish",
    )(near(pieces))


def exchange(pieces, axis):
    return lax.all_to_all(pieces, axis, split_axis=0, concat_axis=0, tiled=True)


def local(batch_sizes, seq_lens, page_table, queries, kv_pool, new_kv, out_weight):
    n_tp = lax.axis_size("tp")
    n_grp = lax.axis_size("grp")
    own = queries[0]
    slots = own.shape[0]

    def from_pair(block, step):
        return lax.ppermute(block, "grp", [(i, i ^ step) for i in range(n_grp)])

    own_block = out_weight.T
    pair = join(own_block, from_pair(own_block, FIRST_STEP))
    pairs = {0: pair, **{step: from_pair(pair, step) for step in PAIR_STEPS}}
    fanned = copies(own, n_tp)
    gathered = exchange(fanned, "tp")
    message = attend(batch_sizes, seq_lens[0], page_table[0], gathered, kv_pool[0])
    received = exchange(message, "tp")
    attended = merge(batch_sizes, received, own, new_kv[0])
    shares = project(attended, pairs, n_tp)
    totals = total_copies(exchange(shares, "tp"))
    return finish(exchange(totals, "tp"), slots, n_grp * out_weight.shape[1])


def solution(mesh):
    return jax.shard_map(
        local,
        mesh=mesh,
        in_specs=(
            P("grp"),
            P("grp", None),
            P("grp", None, "tp"),
            P("grp", None, "tp"),
            P("grp", "tp", None, None),
            P("grp", None, None),
            P("tp", "grp"),
        ),
        out_specs=P("grp", None, None),
        check_vma=False,
    )
```
